256 devices in a mesh: site: 64 (over z, x, core), dom: 4 (over y).
Axes of the slice: x: 4, y: 4, z: 8, core: 2. Of those that a mesh axis runs over, the one named last changes fastest.
Arguments:
- top_partial: float32 [16, 61, 4, 65536], P(None, None, 'dom', 'site'), may hold values from 0.001 to 1
- bottom_partial: float32 [16, 61, 4, 65536], P(None, None, 'dom', 'site'), may hold values from 0.001 to 1
- left_vectors: float32 [256, 61, 61], P('dom'), may hold values from 0.05 to 1
- right_vectors: float32 [256, 61, 61], P('dom'), may hold values from 0.05 to 1
- decay_rates: float32 [256, 61], P('dom'), may hold values from 0.05 to 8
- state_weights: float32 [256, 61], P('dom'), may hold values from 0.002 to 0.05
- part_rates: float32 [256], P('dom'), may hold values from 0.3 to 3
- branch_lengths: float32 [1997], replicated, may hold values from 0.02 to 0.5
- pattern_weights: int32 [4, 65536], P('dom', 'site'), may hold values from 0 to 9
- block_partition: int32 [4, 512], P('dom', 'site'), may hold values from 0 to 255
- chosen_branches: int32 [16], replicated, may hold values from 0 to 1996, as said below
Outputs:
- site_loglik: float32 [16, 4, 65536], P(None, 'dom', 'site')
- part_derivs: float32 [2, 16, 256], P(None, None, 'dom')
- new_lengths: float32 [1997], replicated
The draws below stay inside these ranges and needn't reach their ends.
Inputs may be any that keep to these rules, and one draw needn't show every extreme that they name: `chosen_branches`: distinct branch numbers.
All inputs are finite; a program needn't handle non-finite values.
Results may differ from the reference program's by a relative error of at most 0.0003.
Values sent between devices are 32-bit elements; how exact they have to be, the bound alone decides.
A program may use at most 64 MiB of HBM per device.

```python
import math
import jax
import jax.numpy as jnp
import numpy as np
from jax import lax

STATES = 61
BR = 16
BLK = 128
TREE_BR = 1997
PARTS_SIZE = 256
SG = 65536
NBLK_G = 512
N_DOM = 4


def draw_chosen_branches(key, part):
    picked = jax.random.permutation(jax.random.fold_in(key, 17), TREE_BR)
    return picked[:BR].astype(jnp.int32)


def with_ends(result, key, low, top_value):
    spot = [jax.random.randint(jax.random.fold_in(key, axis), (), 0, length) for axis, length in enumerate(result.shape)]
    longest = result.shape.index(max(result.shape))
    next_to = spot[:longest] + [(spot[longest] + 1) % result.shape[longest]] + spot[longest + 1:]
    return result.at[tuple(spot)].set(low).at[tuple(next_to)].set(top_value)


def block_levels(own_key, dims, shards, least, high):
    def one(position, parts):
        draws = jax.random.uniform(jax.random.fold_in(jax.random.fold_in(own_key, 6), position), (parts,), jnp.float32, least / len(shards), high / len(shards))
        return jnp.repeat(jnp.exp(draws), dims[position] // parts).reshape((-1,) + (1,) * (len(dims) - position - 1))

    level = one(*shards[0])
    for cut in shards[1:]:
        level = level * one(*cut)
    return level


def cumulative_ranks(count, skew):
    loads = [(1 << 20) // math.isqrt(standing ** skew) + 1 for standing in range(1, count + 1)]
    scale = 1 + sum(loads) // (1 << 30)
    return np.cumsum(np.array([max(1, weight // scale) for weight in loads]))


def ranked(key, extent, amount, slope):
    grid = cumulative_ranks(amount, slope)
    ticket = jax.random.randint(jax.random.fold_in(key, 1), extent, 0, int(grid[amount - 1]))
    standing = jnp.searchsorted(jnp.asarray(grid, jnp.int32), ticket, side="right")
    return jax.random.permutation(jax.random.fold_in(key, 2), amount)[standing].astype(jnp.int32)


def setup_inputs(seed: int = 0) -> dict:
    splits = jax.random.split(jax.random.key(seed), 12)
    top_partial = jnp.clip(jnp.exp(math.log(1.0) - 6.9077552 * jax.random.uniform(splits[0], (BR, STATES, N_DOM, SG), jnp.float32) ** block_levels(splits[0], (BR, STATES, N_DOM, SG), ((2, 4), (3, 64)), -0.2, 0.2)), 0.001, 1.0)
    bottom_partial = jnp.clip(jnp.exp(math.log(1.0) - 6.9077552 * jax.random.uniform(splits[1], (BR, STATES, N_DOM, SG), jnp.float32) ** block_levels(splits[1], (BR, STATES, N_DOM, SG), ((2, 4), (3, 64)), -0.2, 0.2)), 0.001, 1.0)
    left_vectors = jnp.clip(0.05 + 0.95 * jax.random.uniform(splits[2], (PARTS_SIZE, STATES, STATES), jnp.float32) ** block_levels(splits[2], (PARTS_SIZE, STATES, STATES), ((0, 4),), -0.2, 0.2), 0.05, 1.0)
    right_vectors = jnp.clip(0.05 + 0.95 * jax.random.uniform(splits[3], (PARTS_SIZE, STATES, STATES), jnp.float32) ** block_levels(splits[3], (PARTS_SIZE, STATES, STATES), ((0, 4),), -0.2, 0.2), 0.05, 1.0)
    decay_rates = jnp.clip(jnp.exp(math.log(8.0) - 5.075174 * jax.random.uniform(splits[4], (PARTS_SIZE, STATES), jnp.float32) ** block_levels(splits[4], (PARTS_SIZE, STATES), ((0, 4),), -0.2, 0.2)), 0.05, 8.0)
    state_weights = jnp.clip(jnp.exp(math.log(0.05) - 3.218876 * jax.random.uniform(splits[5], (PARTS_SIZE, STATES), jnp.float32) ** block_levels(splits[5], (PARTS_SIZE, STATES), ((0, 4),), -0.2, 0.2)), 0.002, 0.05)
    part_rates = jnp.clip(jnp.exp(math.log(3.0) - 2.3025851 * jax.random.uniform(splits[6], (PARTS_SIZE,), jnp.float32) ** block_levels(splits[6], (PARTS_SIZE,), ((0, 4),), -0.2, 0.2)), 0.3, 3.0)
    branch_lengths = jnp.clip(jnp.exp(jax.random.uniform(splits[7], (TREE_BR,), jnp.float32, math.log(0.02), math.log(0.5))), 0.02, 0.5)
    pattern_weights = with_ends(jax.random.randint(splits[8], (N_DOM, SG), 0, 10), jax.random.fold_in(splits[8], 1), 0, 9).astype(jnp.int32)
    block_partition = with_ends(ranked(splits[9], (N_DOM, NBLK_G), PARTS_SIZE, 2), jax.random.fold_in(splits[9], 3), 0, PARTS_SIZE - 1).astype(jnp.int32)
    chosen_branches = draw_chosen_branches(jax.random.fold_in(splits[11], 71), 0)
    return {"top_partial": top_partial, "bottom_partial": bottom_partial, "left_vectors": left_vectors, "right_vectors": right_vectors, "decay_rates": decay_rates, "state_weights": state_weights, "part_rates": part_rates, "branch_lengths": branch_lengths, "pattern_weights": pattern_weights, "block_partition": block_partition, "chosen_branches": chosen_branches}


def project(upper, lower, vec_left, vec_right, state_w):
    scaled = upper * jnp.transpose(state_w)[None, :, :, None]
    lefts = jnp.einsum('binl,nik->bknl', scaled, vec_left, precision=lax.Precision.HIGHEST)
    rights = jnp.einsum('nkj,bjnl->bknl', vec_right, lower, precision=lax.Precision.HIGHEST)
    return lefts, rights


def finish(lefts, rights, exponent, times, weight_f):
    joint = lefts * rights
    expo = jnp.transpose(exponent)[None, :, :, None]
    decayed = joint * jnp.exp(expo * times[:, None, None, None])
    like_zero = jnp.sum(decayed, axis=1)
    like_one = jnp.sum(decayed * expo, axis=1)
    like_two = jnp.sum(decayed * expo * expo, axis=1)
    first = like_one / like_zero
    second = like_two / like_zero - first * first
    loglik = weight_f[None] * jnp.log(like_zero)
    sums = jnp.stack([jnp.sum(weight_f[None] * first, axis=-1), jnp.sum(weight_f[None] * second, axis=-1)])
    return loglik, sums


def reference(top_partial, bottom_partial, left_vectors, right_vectors, decay_rates, state_weights, part_rates, branch_lengths, pattern_weights, block_partition, chosen_branches):
    times = branch_lengths[chosen_branches]
    upper_all = jnp.moveaxis(top_partial, 2, 0)
    lower_all = jnp.moveaxis(bottom_partial, 2, 0)

    def one_group(items):
        upper, lower, weights_g, blocks = items
        nblocks = blocks.shape[0]
        upper = upper.reshape(BR, STATES, nblocks, BLK)
        lower = lower.reshape(BR, STATES, nblocks, BLK)
        vec_left = left_vectors[blocks]
        vec_right = right_vectors[blocks]
        exponent = -decay_rates[blocks] * part_rates[blocks][:, None]
        lefts, rights = project(upper, lower, vec_left, vec_right, state_weights[blocks])
        weight_f = weights_g.astype(jnp.float32).reshape(nblocks, BLK)
        loglik, sums = finish(lefts, rights, exponent, times, weight_f)
        onehot = (blocks[:, None] == jnp.arange(PARTS_SIZE, dtype=jnp.int32)[None, :]).astype(jnp.float32)
        part_sums = jnp.einsum('abn,np->abp', sums, onehot, precision=lax.Precision.HIGHEST)
        return loglik.reshape(BR, nblocks * BLK), part_sums

    logliks, part_all = lax.map(one_group, (upper_all, lower_all, pattern_weights, block_partition))
    site_loglik = jnp.moveaxis(logliks, 0, 1)
    part_derivs = jnp.sum(part_all, axis=0)
    totals = jnp.sum(part_derivs, axis=2)
    updated = times - totals[0] / totals[1]
    new_lengths = branch_lengths.at[chosen_branches].set(updated)
    return site_loglik, part_derivs, new_lengths
```

```python
import functools

import jax
import jax.numpy as jnp
from jax import lax
from jax.experimental import pallas as pl
from jax.experimental.pallas import tpu as pltpu
from jax.sharding import PartitionSpec as P

BLK = 128
STATES = 61
ROWS = 64
BR = 16
F32 = jnp.float32
BF16 = jnp.bfloat16
MESH = pl.DeviceIdType.MESH


def hi_lo(x):
    hi = x.astype(BF16)
    return hi, (x - hi.astype(F32)).astype(BF16)


def three(x):
    hi = x.astype(BF16)
    rest = x - hi.astype(F32)
    mid = rest.astype(BF16)
    return hi, mid, (rest - mid.astype(F32)).astype(BF16)


def dot(a, b, contract):
    return lax.dot_general(a, b, ((contract[0], contract[1]), ((), ())), preferred_element_type=F32)


def step_kernel(
    sizes,
    top_hbm,
    bottom_hbm,
    left_hbm,
    right_hbm,
    decay_hbm,
    weight_hbm,
    rates,
    lengths,
    chosen,
    blocks,
    pattern_hbm,
    loglik_out,
    part_out,
    updated_out,
    top,
    bottom,
    left,
    right,
    decay,
    weight,
    pattern,
    asked,
    send_tab,
    recv_tab,
    likes,
    sums,
    gath,
    zsum,
    local_sem,
    ask_send,
    ask_recv,
    tab_send,
    tab_recv,
    gath_send,
    gath_recv,
    zsum_send,
    zsum_recv,
):
    planes, across, doms, nblk, owned = sizes
    site = lax.axis_index("site")
    me = lax.axis_index("dom")
    plane = site // across
    column = site % across
    group = across * doms
    rank = column * doms + me
    dom_peer = lambda off: lax.rem(me + off, doms)

    def group_peer(off):
        r = lax.rem(rank + off, group)
        return {"site": plane * across + r // doms, "dom": lax.rem(r, doms)}

    def plane_peer(off):
        return {"site": lax.rem(plane + off, planes) * across + column, "dom": me}

    barrier = pltpu.get_barrier_semaphore()

    @pl.loop(1, group)
    def _(off):
        pl.semaphore_signal(barrier, inc=1, device_id=group_peer(off), device_id_type=MESH)

    @pl.loop(1, planes)
    def _(off):
        pl.semaphore_signal(barrier, inc=1, device_id=plane_peer(off), device_id_type=MESH)

    full = STATES * owned
    loads = [
        pltpu.make_async_copy(left_hbm, left.at[pl.ds(0, full)], local_sem.at[0]),
        pltpu.make_async_copy(right_hbm, right.at[pl.ds(0, full)], local_sem.at[1]),
        pltpu.make_async_copy(decay_hbm, decay, local_sem.at[2]),
        pltpu.make_async_copy(weight_hbm, weight, local_sem.at[3]),
        pltpu.make_async_copy(pattern_hbm, pattern, local_sem.at[4]),
        pltpu.make_async_copy(top_hbm, top.at[pl.ds(0, BR * STATES * nblk)], local_sem.at[5]),
        pltpu.make_async_copy(bottom_hbm, bottom.at[pl.ds(0, BR * STATES * nblk)], local_sem.at[6]),
    ]
    for load in loads:
        load.start()
    tail = (ROWS - STATES) * owned
    left[pl.ds(full, tail), :] = jnp.zeros((tail, STATES), F32)
    right[pl.ds(full, tail), :] = jnp.zeros((tail, STATES), F32)
    tail = (ROWS - STATES) * nblk
    top[pl.ds(BR * STATES * nblk, tail), :] = jnp.zeros((tail, BLK), F32)
    bottom[pl.ds(BR * STATES * nblk, tail), :] = jnp.zeros((tail, BLK), F32)

    pl.semaphore_wait(barrier, group + planes - 2)

    def ask(off):
        return pltpu.make_async_remote_copy(
            src_ref=blocks,
            dst_ref=asked.at[off - 1],
            send_sem=ask_send.at[off - 1],
            recv_sem=ask_recv.at[off - 1],
            device_id={"site": site, "dom": dom_peer(off)},
            device_id_type=MESH,
        )

    for off in range(1, doms):
        ask(off).start()

    row_id = lax.broadcasted_iota(jnp.int32, (ROWS, ROWS), 0)

    def entry(part):
        relative = part - me * owned
        inside = jnp.logical_and(relative >= 0, relative < owned).astype(F32)
        at = jnp.clip(relative, 0, owned - 1)
        lv = jnp.pad(left[pl.ds(at, ROWS, stride=owned), :], ((0, 0), (0, ROWS - STATES)))
        rv = jnp.pad(right[pl.ds(at, ROWS, stride=owned), :], ((0, 0), (0, ROWS - STATES)))
        pad = lambda x: jnp.pad(x, ((0, 0), (0, ROWS - STATES)))
        exponent = pad(-decay[pl.ds(at, 1), :] * rates[at])
        state_w = pad(weight[pl.ds(at, 1), :])
        lv = jnp.where(row_id == STATES, exponent, jnp.where(row_id == STATES + 1, state_w, lv))
        return jnp.concatenate([lv, rv], axis=1) * inside

    def tab(off, n):
        return pltpu.make_async_remote_copy(
            src_ref=send_tab.at[off - 1, n],
            dst_ref=recv_tab.at[off - 1, n],
            send_sem=tab_send.at[off - 1, n],
            recv_sem=tab_recv.at[off - 1, n],
            device_id={"site": site, "dom": dom_peer(off)},
            device_id_type=MESH,
        )

    for load in loads[:4]:
        load.wait()
    for off in range(1, doms):
        ask(off).wait_recv()

    @pl.loop(0, nblk)
    def _(n):
        for off in range(1, doms):
            send_tab[off - 1, n] = entry(asked[doms - off - 1, 0, n])
        for off in range(1, doms):
            tab(off, n).start()

    for load in loads[4:]:
        load.wait()

    lane64 = lax.broadcasted_iota(jnp.int32, (ROWS, ROWS), 1)

    @pl.loop(0, nblk)
    def _(n):
        got = entry(blocks[0, n])
        for off in range(1, doms):
            tab(off, n).wait_recv()
            got = got + recv_tab[off - 1, n]
        lv_t = jnp.transpose(got[:, :ROWS])
        exponent = lv_t[:, STATES : STATES + 1]
        state_w = lv_t[:, STATES + 1 : STATES + 2]
        lv_t = jnp.where(lane64 < STATES, lv_t, 0.0)
        lv_hi, lv_lo = hi_lo(lv_t)
        rv_hi, rv_lo = hi_lo(got[:, ROWS:])
        lhs_l = jnp.concatenate([lv_hi, lv_hi, lv_lo], axis=1)
        lhs_r = jnp.concatenate([rv_hi, rv_hi, rv_lo], axis=1)
        expo_b = jnp.broadcast_to(exponent, (ROWS, BLK))
        w_b = jnp.broadcast_to(state_w, (ROWS, BLK))

        def stacked(ref, b, scale):
            x = ref[pl.ds(b * (STATES * nblk) + n, ROWS, stride=nblk), :]
            if scale is not None:
                x = x * scale
            hi, lo = hi_lo(x)
            return jnp.concatenate([hi, lo, hi], axis=0)

        for b in range(0, BR, 2):
            x = jnp.concatenate([stacked(top, b, w_b), stacked(top, b + 1, w_b)], axis=1)
            y = jnp.concatenate([stacked(bottom, b, None), stacked(bottom, b + 1, None)], axis=1)
            joint = dot(lhs_l, x, ((1,), (0,))) * dot(lhs_r, y, ((1,), (0,)))
            for c in range(2):
                time = lengths[chosen[b + c]]
                decayed = joint[:, c * BLK : (c + 1) * BLK] * jnp.exp(expo_b * time)
                for power in range(3):
                    likes[power, pl.ds(b + c, 1), :] = jnp.sum(decayed, axis=0, keepdims=True)
                    if power < 2:
                        decayed = decayed * expo_b
        like0 = likes[0]
        first = likes[1] / like0
        second = likes[2] / like0 - first * first
        sites_w = pattern[pl.ds(n, 1), :].astype(F32)
        loglik_out[n] = sites_w * jnp.log(like0)
        sums[pl.ds(n * 32, BR), :] = sites_w * first
        sums[pl.ds(n * 32 + BR, BR), :] = sites_w * second

    ones = jnp.ones((8, BLK), BF16)
    total = sum(dot(ones, piece, ((1,), (1,))) for piece in three(sums[...]))
    lane_blk = lax.broadcasted_iota(jnp.int32, (1, BLK), 1) // 32
    for g in range(2):
        gath[rank, pl.ds(g, 1), :] = total[0:1, g * BLK : (g + 1) * BLK]
        ids = jnp.zeros((1, BLK), F32)
        for k in range(4):
            ids = jnp.where(lane_blk == k, blocks[0, g * 4 + k].astype(F32), ids)
        gath[rank, pl.ds(2 + g, 1), :] = ids

    def give(off):
        return pltpu.make_async_remote_copy(
            src_ref=gath.at[rank],
            dst_ref=gath.at[rank],
            send_sem=gath_send.at[off],
            recv_sem=gath_recv.at[off],
            device_id=group_peer(off),
            device_id_type=MESH,
        )

    @pl.loop(1, group)
    def _(off):
        give(off).start()

    @pl.loop(1, group)
    def _(off):
        give(off).wait_recv()

    vals = jnp.concatenate([gath[:, 0, :], gath[:, 1, :]], axis=0)
    ids = jnp.concatenate([gath[:, 2, :], gath[:, 3, :]], axis=0)
    local = lax.broadcasted_iota(jnp.int32, (2 * group, BLK), 1)
    mine = jnp.where(local < owned, local + me * owned, -1).astype(F32)
    hot = jnp.concatenate(
        [(ids[:, k * 32 : k * 32 + 1] == mine).astype(F32).astype(BF16) for k in range(4)], axis=1
    )
    vals_t = jnp.transpose(vals)
    spread = dot(
        jnp.concatenate(three(vals_t), axis=1),
        jnp.concatenate([hot, hot, hot], axis=0),
        ((1,), (0,)),
    )
    by_part = sum(spread[k * 32 : (k + 1) * 32, k * BLK : (k + 1) * BLK] for k in range(4))
    lane = lax.broadcasted_iota(jnp.int32, (BR, BLK), 1)
    zsum[plane, 0:BR, :] = jnp.where(
        lane < owned, by_part[:BR], pltpu.roll(by_part[BR:], owned, 1)
    )
    column_sum = jnp.sum(vals, axis=0, keepdims=True)
    all_sum = column_sum
    for k in range(1, 4):
        all_sum = all_sum + pltpu.roll(column_sum, 32 * k, 1)
    zsum[plane, BR : BR + 8, :] = jnp.broadcast_to(all_sum, (8, BLK))

    def pass_on(off):
        return pltpu.make_async_remote_copy(
            src_ref=zsum.at[plane],
            dst_ref=zsum.at[plane],
            send_sem=zsum_send.at[off],
            recv_sem=zsum_recv.at[off],
            device_id=plane_peer(off),
            device_id_type=MESH,
        )

    @pl.loop(1, planes)
    def _(off):
        pass_on(off).start()

    @pl.loop(1, planes)
    def _(off):
        pass_on(off).wait_recv()

    done = jnp.sum(zsum[...], axis=0)
    both = done[:BR]
    part_out[0] = both[:, :owned]
    part_out[1] = pltpu.roll(both, owned, 1)[:, :owned]
    totals = done[BR : BR + 8]
    lane8 = lax.broadcasted_iota(jnp.int32, (8, BLK), 1)
    times = jnp.zeros((8, BLK), F32)
    for b in range(BR):
        times = jnp.where(lane8 == b, lengths[chosen[b]], times)
    updated_out[...] = times - totals / pltpu.roll(totals, BLK - BR, 1)

    for off in range(1, doms):
        ask(off).wait_send()

        @pl.loop(0, nblk)
        def _(n):
            tab(off, n).wait_send()

    @pl.loop(1, group)
    def _(off):
        give(off).wait_send()

    @pl.loop(1, planes)
    def _(off):
        pass_on(off).wait_send()


def on_device(
    sizes,
    top_partial,
    bottom_partial,
    left_vectors,
    right_vectors,
    decay_rates,
    state_weights,
    part_rates,
    branch_lengths,
    pattern_weights,
    block_partition,
    chosen_branches,
):
    planes, across, doms, nblk, owned = sizes
    flat = BR * STATES * nblk
    group = across * doms
    anywhere = pl.BlockSpec(memory_space=pl.ANY)
    scalars = pl.BlockSpec(memory_space=pltpu.SMEM)
    vmem = pl.BlockSpec(memory_space=pltpu.VMEM)
    loglik, share, updated = pl.pallas_call(
        functools.partial(step_kernel, sizes),
        out_shape=(
            jax.ShapeDtypeStruct((nblk, BR, BLK), F32),
            jax.ShapeDtypeStruct((2, BR, owned), F32),
            jax.ShapeDtypeStruct((8, BLK), F32),
        ),
        in_specs=[anywhere] * 6 + [scalars] * 4 + [anywhere],
        out_specs=(vmem, vmem, vmem),
        scratch_shapes=[
            pltpu.VMEM((flat + (ROWS - STATES) * nblk, BLK), F32),
            pltpu.VMEM((flat + (ROWS - STATES) * nblk, BLK), F32),
            pltpu.VMEM((ROWS * owned, STATES), F32),
            pltpu.VMEM((ROWS * owned, STATES), F32),
            pltpu.VMEM((owned, STATES), F32),
            pltpu.VMEM((owned, STATES), F32),
            pltpu.VMEM((nblk, BLK), jnp.int32),
            pltpu.SMEM((doms - 1, 1, nblk), jnp.int32),
            pltpu.VMEM((doms - 1, nblk, ROWS, BLK), F32),
            pltpu.VMEM((doms - 1, nblk, ROWS, BLK), F32),
            pltpu.VMEM((3, BR, BLK), F32),
            pltpu.VMEM((32 * nblk, BLK), F32),
            pltpu.VMEM((group, 4, BLK), F32),
            pltpu.VMEM((planes, BR + 8, BLK), F32),
            pltpu.SemaphoreType.DMA((7,)),
            pltpu.SemaphoreType.DMA((doms - 1,)),
            pltpu.SemaphoreType.DMA((doms - 1,)),
            pltpu.SemaphoreType.DMA((doms - 1, nblk)),
            pltpu.SemaphoreType.DMA((doms - 1, nblk)),
            pltpu.SemaphoreType.DMA((group,)),
            pltpu.SemaphoreType.DMA((group,)),
            pltpu.SemaphoreType.DMA((planes,)),
            pltpu.SemaphoreType.DMA((planes,)),
        ],
        compiler_params=pltpu.CompilerParams(
            collective_id=0, has_side_effects=True, vmem_limit_bytes=40 * 1024 * 1024
        ),
    )(
        top_partial.reshape(BR, STATES, nblk, BLK).reshape(flat, BLK),
        bottom_partial.reshape(BR, STATES, nblk, BLK).reshape(flat, BLK),
        jnp.transpose(left_vectors, (1, 0, 2)).reshape(STATES * owned, STATES),
        jnp.transpose(right_vectors, (1, 0, 2)).reshape(STATES * owned, STATES),
        decay_rates,
        state_weights,
        part_rates,
        branch_lengths,
        chosen_branches,
        block_partition,
        pattern_weights.reshape(nblk, BLK),
    )
    new_lengths = branch_lengths.at[chosen_branches].set(updated[0, :BR])
    loglik = jnp.transpose(loglik, (1, 0, 2)).reshape(BR, 1, nblk * BLK)
    return (loglik, share, new_lengths)


def solution(mesh):
    sites, doms = mesh.shape["site"], mesh.shape["dom"]
    across = 8 if sites % 8 == 0 and sites > 8 else 2
    sizes = (sites // across, across, doms, 8, 256 // doms)
    return jax.shard_map(
        functools.partial(on_device, sizes),
        mesh=mesh,
        in_specs=(
            P(None, None, "dom", "site"),
            P(None, None, "dom", "site"),
            P("dom", None, None),
            P("dom", None, None),
            P("dom", None),
            P("dom", None),
            P("dom"),
            P(),
            P("dom", "site"),
            P("dom", "site"),
            P(),
        ),
        out_specs=(P(None, "dom", "site"), P(None, None, "dom"), P()),
        check_vma=False,
    )
```

```python
import functools

import jax
import jax.numpy as jnp
from jax import lax
from jax.experimental import pallas as pl
from jax.experimental.pallas import tpu as pltpu
from jax.sharding import PartitionSpec as P

BLK = 128
STATES = 61
ROWS = 64
BR = 16
F32 = jnp.float32
BF16 = jnp.bfloat16
MESH = pl.DeviceIdType.MESH


def hi_lo(x):
    hi = x.astype(BF16)
    return hi, (x - hi.astype(F32)).astype(BF16)


def three(x):
    hi = x.astype(BF16)
    rest = x - hi.astype(F32)
    mid = rest.astype(BF16)
    return hi, mid, (rest - mid.astype(F32)).astype(BF16)


def dot(a, b, contract):
    return lax.dot_general(a, b, ((contract[0], contract[1]), ((), ())), preferred_element_type=F32)


def step_kernel(
    sizes,
    top_hbm,
    bottom_hbm,
    left_hbm,
    right_hbm,
    decay_hbm,
    weight_hbm,
    rates_hbm,
    lengths_hbm,
    chosen_hbm,
    blocks_hbm,
    pattern_hbm,
    loglik_out,
    part_out,
    lengths_out,
    top,
    bottom,
    left,
    right,
    decay,
    weight,
    pattern,
    rates,
    lengths,
    chosen,
    blocks,
    lengths_v,
    asked,
    send_tab,
    recv_tab,
    likes,
    sums,
    gath,
    zsum,
    local_sem,
    ask_send,
    ask_recv,
    tab_send,
    tab_recv,
    gath_send,
    gath_recv,
    zsum_send,
    zsum_recv,
):
    planes, across, doms, nblk, owned = sizes
    site = lax.axis_index("site")
    me = lax.axis_index("dom")
    plane = site // across
    column = site % across
    group = across * doms
    rank = column * doms + me
    dom_at = [me] + [lax.rem(me + off, doms) for off in range(1, doms)]
    dom_peer = lambda off: dom_at[off]
    site_at = [site] + [plane * across + lax.rem(column + off, across) for off in range(1, across)]
    plane_at = [site] + [lax.rem(plane + off, planes) * across + column for off in range(1, planes)]

    def group_peer(off):
        return {"site": site_at[off // doms], "dom": dom_at[off % doms]}

    def plane_peer(off):
        return {"site": plane_at[off], "dom": me}

    barrier = pltpu.get_barrier_semaphore()
    far = sorted(range(1, group), key=lambda off: -min(off // doms, across - off // doms))
    for off in sorted(range(1, planes), key=lambda off: -min(off, planes - off)):
        pl.semaphore_signal(barrier, inc=1, device_id=plane_peer(off), device_id_type=MESH)
    for off in far:
        pl.semaphore_signal(barrier, inc=1, device_id=group_peer(off), device_id_type=MESH)

    full = STATES * owned
    small = [
        pltpu.make_async_copy(blocks_hbm, blocks, local_sem.at[7]),
        pltpu.make_async_copy(rates_hbm, rates, local_sem.at[8]),
        pltpu.make_async_copy(chosen_hbm, chosen, local_sem.at[9]),
        pltpu.make_async_copy(lengths_hbm, lengths, local_sem.at[10]),
    ]
    small.append(pltpu.make_async_copy(lengths_hbm, lengths_v, local_sem.at[11]))
    small[0].start()
    loads = [
        pltpu.make_async_copy(left_hbm, left.at[pl.ds(0, full)], local_sem.at[0]),
        pltpu.make_async_copy(right_hbm, right.at[pl.ds(0, full)], local_sem.at[1]),
        pltpu.make_async_copy(decay_hbm, decay, local_sem.at[2]),
        pltpu.make_async_copy(weight_hbm, weight, local_sem.at[3]),
        pltpu.make_async_copy(pattern_hbm, pattern, local_sem.at[4]),
        pltpu.make_async_copy(top_hbm, top.at[pl.ds(0, BR * STATES * nblk)], local_sem.at[5]),
        pltpu.make_async_copy(bottom_hbm, bottom.at[pl.ds(0, BR * STATES * nblk)], local_sem.at[6]),
    ]
    for load in loads[:4] + small[1:] + loads[4:]:
        load.start()
    tail = (ROWS - STATES) * owned
    left[pl.ds(full, tail), :] = jnp.zeros((tail, STATES), F32)
    right[pl.ds(full, tail), :] = jnp.zeros((tail, STATES), F32)
    tail = (ROWS - STATES) * nblk
    top[pl.ds(BR * STATES * nblk, tail), :] = jnp.zeros((tail, BLK), F32)
    bottom[pl.ds(BR * STATES * nblk, tail), :] = jnp.zeros((tail, BLK), F32)

    small[0].wait()
    pl.semaphore_wait(barrier, group + planes - 2)

    def ask(off):
        return pltpu.make_async_remote_copy(
            src_ref=blocks,
            dst_ref=asked.at[off - 1],
            send_sem=ask_send.at[off - 1],
            recv_sem=ask_recv.at[off - 1],
            device_id={"site": site, "dom": dom_peer(off)},
            device_id_type=MESH,
        )

    for off in range(1, doms):
        ask(off).start()

    row_id = lax.broadcasted_iota(jnp.int32, (ROWS, ROWS), 0)

    def entry(part):
        relative = part - me * owned
        inside = jnp.logical_and(relative >= 0, relative < owned).astype(F32)
        at = jnp.clip(relative, 0, owned - 1)
        lv = jnp.pad(left[pl.ds(at, ROWS, stride=owned), :], ((0, 0), (0, ROWS - STATES)))
        rv = jnp.pad(right[pl.ds(at, ROWS, stride=owned), :], ((0, 0), (0, ROWS - STATES)))
        pad = lambda x: jnp.pad(x, ((0, 0), (0, ROWS - STATES)))
        exponent = pad(-decay[pl.ds(at, 1), :] * rates[at])
        state_w = pad(weight[pl.ds(at, 1), :])
        lv = jnp.where(row_id == STATES, exponent, jnp.where(row_id == STATES + 1, state_w, lv))
        return jnp.concatenate([lv, rv], axis=1) * inside

    def tab(off, n):
        return pltpu.make_async_remote_copy(
            src_ref=send_tab.at[off - 1, n],
            dst_ref=recv_tab.at[off - 1, n],
            send_sem=tab_send.at[off - 1, n],
            recv_sem=tab_recv.at[off - 1, n],
            device_id={"site": site, "dom": dom_peer(off)},
            device_id_type=MESH,
        )

    for load in loads[:4] + small[1:]:
        load.wait()
    for off in range(1, doms):
        ask(off).wait_recv()

    @pl.loop(0, nblk)
    def _(n):
        for off in range(1, doms):
            send_tab[off - 1, n] = entry(asked[doms - off - 1, 0, n])
        for off in range(1, doms):
            tab(off, n).start()

    for load in loads[4:]:
        load.wait()

    lane64 = lax.broadcasted_iota(jnp.int32, (ROWS, ROWS), 1)

    @pl.loop(0, nblk)
    def _(n):
        got = entry(blocks[0, n])
        for off in range(1, doms):
            tab(off, n).wait_recv()
            got = got + recv_tab[off - 1, n]
        lv_t = jnp.transpose(got[:, :ROWS])
        exponent = lv_t[:, STATES : STATES + 1]
        state_w = lv_t[:, STATES + 1 : STATES + 2]
        lv_t = jnp.where(lane64 < STATES, lv_t, 0.0)
        lv_hi, lv_lo = hi_lo(lv_t)
        rv_hi, rv_lo = hi_lo(got[:, ROWS:])
        lhs_l = jnp.concatenate([lv_hi, lv_hi, lv_lo], axis=1)
        lhs_r = jnp.concatenate([rv_hi, rv_hi, rv_lo], axis=1)
        expo_b = jnp.broadcast_to(exponent, (ROWS, BLK))
        w_b = jnp.broadcast_to(state_w, (ROWS, BLK))

        def stacked(ref, b, scale):
            x = ref[pl.ds(b * (STATES * nblk) + n, ROWS, stride=nblk), :]
            if scale is not None:
                x = x * scale
            hi, lo = hi_lo(x)
            return jnp.concatenate([hi, lo, hi], axis=0)

        for b in range(0, BR, 2):
            x = jnp.concatenate([stacked(top, b, w_b), stacked(top, b + 1, w_b)], axis=1)
            y = jnp.concatenate([stacked(bottom, b, None), stacked(bottom, b + 1, None)], axis=1)
            joint = dot(lhs_l, x, ((1,), (0,))) * dot(lhs_r, y, ((1,), (0,)))
            for c in range(2):
                time = lengths[chosen[b + c]]
                decayed = joint[:, c * BLK : (c + 1) * BLK] * jnp.exp(expo_b * time)
                for power in range(3):
                    likes[power, pl.ds(b + c, 1), :] = jnp.sum(decayed, axis=0, keepdims=True)
                    if power < 2:
                        decayed = decayed * expo_b
        like0 = likes[0]
        first = likes[1] / like0
        second = likes[2] / like0 - first * first
        sites_w = pattern[pl.ds(n, 1), :].astype(F32)
        loglik_out[pl.ds(n, BR, stride=nblk), :] = sites_w * jnp.log(like0)
        sums[pl.ds(n * 32, BR), :] = sites_w * first
        sums[pl.ds(n * 32 + BR, BR), :] = sites_w * second

    ones = jnp.ones((8, BLK), BF16)
    total = sum(dot(ones, piece, ((1,), (1,))) for piece in three(sums[...]))
    lane_blk = lax.broadcasted_iota(jnp.int32, (1, BLK), 1) // 32
    for g in range(2):
        gath[rank, pl.ds(g, 1), :] = total[0:1, g * BLK : (g + 1) * BLK]
        ids = jnp.zeros((1, BLK), F32)
        for k in range(4):
            ids = jnp.where(lane_blk == k, blocks[0, g * 4 + k].astype(F32), ids)
        gath[rank, pl.ds(2 + g, 1), :] = ids

    def give(off):
        return pltpu.make_async_remote_copy(
            src_ref=gath.at[rank],
            dst_ref=gath.at[rank],
            send_sem=gath_send.at[off],
            recv_sem=gath_recv.at[off],
            device_id=group_peer(off),
            device_id_type=MESH,
        )

    for off in range(1, group):
        give(off).start()

    for off in range(1, group):
        give(off).wait_recv()

    vals = jnp.concatenate([gath[:, 0, :], gath[:, 1, :]], axis=0)
    ids = jnp.concatenate([gath[:, 2, :], gath[:, 3, :]], axis=0)
    local = lax.broadcasted_iota(jnp.int32, (2 * group, BLK), 1)
    mine = jnp.where(local < owned, local + me * owned, -1).astype(F32)
    hot = jnp.concatenate(
        [(ids[:, k * 32 : k * 32 + 1] == mine).astype(F32).astype(BF16) for k in range(4)], axis=1
    )
    vals_t = jnp.transpose(vals)
    spread = dot(
        jnp.concatenate(three(vals_t), axis=1),
        jnp.concatenate([hot, hot, hot], axis=0),
        ((1,), (0,)),
    )
    by_part = sum(spread[k * 32 : (k + 1) * 32, k * BLK : (k + 1) * BLK] for k in range(4))
    lane = lax.broadcasted_iota(jnp.int32, (BR, BLK), 1)
    zsum[plane, 0:BR, :] = jnp.where(
        lane < owned, by_part[:BR], pltpu.roll(by_part[BR:], owned, 1)
    )
    column_sum = jnp.sum(vals, axis=0, keepdims=True)
    all_sum = column_sum
    for k in range(1, 4):
        all_sum = all_sum + pltpu.roll(column_sum, 32 * k, 1)
    zsum[plane, BR : BR + 8, :] = jnp.broadcast_to(all_sum, (8, BLK))

    def pass_on(off):
        return pltpu.make_async_remote_copy(
            src_ref=zsum.at[plane],
            dst_ref=zsum.at[plane],
            send_sem=zsum_send.at[off],
            recv_sem=zsum_recv.at[off],
            device_id=plane_peer(off),
            device_id_type=MESH,
        )

    for off in range(1, planes):
        pass_on(off).start()

    for off in range(1, planes):
        pass_on(off).wait_recv()

    done = jnp.sum(zsum[...], axis=0)
    both = done[:BR]
    part_out[0] = both[:, :owned]
    part_out[1] = pltpu.roll(both, owned, 1)[:, :owned]
    totals = done[BR : BR + 8]
    lane8 = lax.broadcasted_iota(jnp.int32, (8, BLK), 1)
    times = jnp.zeros((8, BLK), F32)
    for b in range(BR):
        times = jnp.where(lane8 == b, lengths[chosen[b]], times)
    updated = times - totals / pltpu.roll(totals, BLK - BR, 1)
    tree = lengths_v.shape[0]
    index = lax.broadcasted_iota(jnp.int32, (1, BLK), 1)
    spots = [jnp.broadcast_to(updated[0:1, b : b + 1], (1, BLK)) for b in range(BR)]
    for start in range(0, tree, BLK):
        width = min(BLK, tree - start)
        new = lengths_v[pl.ds(start, width)].reshape(1, width)
        for b in range(BR):
            new = jnp.where(index[:, :width] + start == chosen[b], spots[b][:, :width], new)
        lengths_out[pl.ds(start, width)] = new.reshape(width)

    for off in range(1, doms):
        ask(off).wait_send()

        @pl.loop(0, nblk)
        def _(n):
            tab(off, n).wait_send()

    for off in range(1, group):
        give(off).wait_send()

    for off in range(1, planes):
        pass_on(off).wait_send()


def store_kernel(loglik, share, lengths, loglik_out, share_out, lengths_out, sem):
    copies = [
        pltpu.make_async_copy(loglik, loglik_out, sem.at[0]),
        pltpu.make_async_copy(share, share_out, sem.at[1]),
        pltpu.make_async_copy(lengths, lengths_out, sem.at[2]),
    ]
    for copy in copies:
        copy.start()
    for copy in copies:
        copy.wait()


def on_device(
    sizes,
    top_partial,
    bottom_partial,
    left_vectors,
    right_vectors,
    decay_rates,
    state_weights,
    part_rates,
    branch_lengths,
    pattern_weights,
    block_partition,
    chosen_branches,
):
    planes, across, doms, nblk, owned = sizes
    flat = BR * STATES * nblk
    group = across * doms
    hbm = pl.BlockSpec(memory_space=pltpu.HBM)
    tree = branch_lengths.shape[0]
    vmem = pl.BlockSpec(memory_space=pltpu.VMEM)
    loglik, share, lengths = pl.pallas_call(
        functools.partial(step_kernel, sizes),
        out_shape=(
            jax.ShapeDtypeStruct((BR * nblk, BLK), F32),
            jax.ShapeDtypeStruct((2, BR, owned), F32),
            jax.ShapeDtypeStruct((tree,), F32),
        ),
        in_specs=[hbm] * 11,
        out_specs=(vmem, vmem, vmem),
        scratch_shapes=[
            pltpu.VMEM((flat + (ROWS - STATES) * nblk, BLK), F32),
            pltpu.VMEM((flat + (ROWS - STATES) * nblk, BLK), F32),
            pltpu.VMEM((ROWS * owned, STATES), F32),
            pltpu.VMEM((ROWS * owned, STATES), F32),
            pltpu.VMEM((owned, STATES), F32),
            pltpu.VMEM((owned, STATES), F32),
            pltpu.VMEM((nblk, BLK), jnp.int32),
            pltpu.SMEM((owned,), F32),
            pltpu.SMEM((tree,), F32),
            pltpu.SMEM((BR,), jnp.int32),
            pltpu.SMEM((1, nblk), jnp.int32),
            pltpu.VMEM((tree,), F32),
            pltpu.SMEM((doms - 1, 1, nblk), jnp.int32),
            pltpu.VMEM((doms - 1, nblk, ROWS, BLK), F32),
            pltpu.VMEM((doms - 1, nblk, ROWS, BLK), F32),
            pltpu.VMEM((3, BR, BLK), F32),
            pltpu.VMEM((32 * nblk, BLK), F32),
            pltpu.VMEM((group, 4, BLK), F32),
            pltpu.VMEM((planes, BR + 8, BLK), F32),
            pltpu.SemaphoreType.DMA((12,)),
            pltpu.SemaphoreType.DMA((doms - 1,)),
            pltpu.SemaphoreType.DMA((doms - 1,)),
            pltpu.SemaphoreType.DMA((doms - 1, nblk)),
            pltpu.SemaphoreType.DMA((doms - 1, nblk)),
            pltpu.SemaphoreType.DMA((group,)),
            pltpu.SemaphoreType.DMA((group,)),
            pltpu.SemaphoreType.DMA((planes,)),
            pltpu.SemaphoreType.DMA((planes,)),
        ],
        compiler_params=pltpu.CompilerParams(
            collective_id=0, has_side_effects=True
        ),
    )(
        top_partial.reshape(BR, STATES, nblk, BLK).reshape(flat, BLK),
        bottom_partial.reshape(BR, STATES, nblk, BLK).reshape(flat, BLK),
        jnp.transpose(left_vectors, (1, 0, 2)).reshape(STATES * owned, STATES),
        jnp.transpose(right_vectors, (1, 0, 2)).reshape(STATES * owned, STATES),
        decay_rates,
        state_weights,
        part_rates,
        branch_lengths,
        chosen_branches,
        block_partition,
        pattern_weights.reshape(nblk, BLK),
    )
    loglik, share, new_lengths = pl.pallas_call(
        store_kernel,
        out_shape=(
            jax.ShapeDtypeStruct((BR * nblk, BLK), F32),
            jax.ShapeDtypeStruct((2, BR, owned), F32),
            jax.ShapeDtypeStruct((tree,), F32),
        ),
        in_specs=[vmem] * 3,
        out_specs=(hbm, hbm, hbm),
        scratch_shapes=[pltpu.SemaphoreType.DMA((3,))],
    )(loglik, share, lengths)
    return (loglik.reshape(BR, 1, nblk * BLK), share, new_lengths)


def solution(mesh):
    sites, doms = mesh.shape["site"], mesh.shape["dom"]
    across = 8 if sites % 8 == 0 and sites > 8 else 2
    sizes = (sites // across, across, doms, 8, 256 // doms)
    return jax.shard_map(
        functools.partial(on_device, sizes),
        mesh=mesh,
        in_specs=(
            P(None, None, "dom", "site"),
            P(None, None, "dom", "site"),
            P("dom", None, None),
            P("dom", None, None),
            P("dom", None),
            P("dom", None),
            P("dom"),
            P(),
            P("dom", "site"),
            P("dom", "site"),
            P(),
        ),
        out_specs=(P(None, "dom", "site"), P(None, None, "dom"), P()),
        check_vma=False,
    )
```

```python
import functools

import jax
import jax.numpy as jnp
from jax import lax
from jax.experimental import pallas as pl
from jax.experimental.pallas import tpu as pltpu
from jax.sharding import PartitionSpec as P

BLK = 128
STATES = 61
ROWS = 64
BR = 16
F32 = jnp.float32
BF16 = jnp.bfloat16
MESH = pl.DeviceIdType.MESH


def hi_lo(x):
    hi = x.astype(BF16)
    return hi, (x - hi.astype(F32)).astype(BF16)


def three(x):
    hi = x.astype(BF16)
    rest = x - hi.astype(F32)
    mid = rest.astype(BF16)
    return hi, mid, (rest - mid.astype(F32)).astype(BF16)


def dot(a, b, contract):
    return lax.dot_general(a, b, ((contract[0], contract[1]), ((), ())), preferred_element_type=F32)


def step_kernel(
    sizes,
    top_hbm,
    bottom_hbm,
    left_hbm,
    right_hbm,
    decay_hbm,
    weight_hbm,
    rates_hbm,
    lengths_hbm,
    chosen_hbm,
    blocks_hbm,
    pattern_hbm,
    loglik_out,
    part_out,
    lengths_out,
    loglik_v,
    part_v,
    new_v,
    top,
    bottom,
    top_s,
    bottom_s,
    own_tab,
    left,
    right,
    decay,
    weight,
    pattern,
    rates,
    lengths,
    chosen,
    blocks,
    lengths_v,
    asked,
    near_tab,
    far_tab,
    recv_tab,
    relay,
    likes,
    sums,
    gath,
    zsum,
    local_sem,
    ask_send,
    ask_recv,
    near_send,
    near_recv,
    far_send,
    far_recv,
    gath_send,
    gath_recv,
    zsum_send,
    zsum_recv,
    line_sem,
    next_sem,
    after_sem,
):
    planes, across, doms, nblk, owned = sizes
    site = lax.axis_index("site")
    me = lax.axis_index("dom")
    plane = site // across
    column = site % across
    group = across * doms
    rank = column * doms + me
    dom_at = [me] + [lax.rem(me + off, doms) for off in range(1, doms)]
    dom_peer = lambda off: dom_at[off]
    site_at = [site] + [plane * across + lax.rem(column + off, across) for off in range(1, across)]
    plane_at = [site] + [lax.rem(plane + off, planes) * across + column for off in range(1, planes)]

    def group_peer(off):
        return {"site": site_at[off // doms], "dom": dom_at[off % doms]}

    def plane_peer(off):
        return {"site": plane_at[off], "dom": me}

    small = [
        pltpu.make_async_copy(blocks_hbm, blocks, local_sem.at[7]),
        pltpu.make_async_copy(rates_hbm, rates, local_sem.at[8]),
        pltpu.make_async_copy(chosen_hbm, chosen, local_sem.at[9]),
        pltpu.make_async_copy(lengths_hbm, lengths, local_sem.at[10]),
    ]
    small.append(pltpu.make_async_copy(lengths_hbm, lengths_v, local_sem.at[11]))
    small[0].start()
    loads = [
        pltpu.make_async_copy(left_hbm, left.at[pl.ds(0, STATES), pl.ds(0, owned)], local_sem.at[0]),
        pltpu.make_async_copy(right_hbm, right.at[pl.ds(0, STATES), pl.ds(0, owned)], local_sem.at[1]),
        pltpu.make_async_copy(decay_hbm, decay, local_sem.at[2]),
        pltpu.make_async_copy(weight_hbm, weight, local_sem.at[3]),
        pltpu.make_async_copy(pattern_hbm, pattern, local_sem.at[4]),
        pltpu.make_async_copy(top_hbm, top.at[pl.ds(0, BR * STATES * nblk)], local_sem.at[5]),
        pltpu.make_async_copy(bottom_hbm, bottom.at[pl.ds(0, BR * STATES * nblk)], local_sem.at[6]),
    ]
    for load in loads[:4] + small[1:] + loads[4:]:
        load.start()

    barrier = pltpu.get_barrier_semaphore()
    here = lambda s: {"site": s, "dom": me}
    near = [{"site": site, "dom": d} for d in dom_at[1:]]
    near += [here(s) for s in site_at[1:]] + [here(plane_at[1]), here(plane_at[planes - 1])]
    for device in near:
        pl.semaphore_signal(barrier, inc=1, device_id=device, device_id_type=MESH)
    pitch = left.shape[1]
    tail = (ROWS - STATES, pitch, STATES)
    left[pl.ds(STATES, ROWS - STATES)] = jnp.zeros(tail, F32)
    right[pl.ds(STATES, ROWS - STATES)] = jnp.zeros(tail, F32)
    left_rows = left.reshape(ROWS * pitch, STATES)
    right_rows = right.reshape(ROWS * pitch, STATES)
    tail = (ROWS - STATES) * nblk
    top[pl.ds(BR * STATES * nblk, tail), :] = jnp.zeros((tail, BLK), F32)
    bottom[pl.ds(BR * STATES * nblk, tail), :] = jnp.zeros((tail, BLK), F32)

    small[0].wait()
    pl.semaphore_wait(barrier, len(near))

    def ask(off):
        return pltpu.make_async_remote_copy(
            src_ref=blocks,
            dst_ref=asked.at[off - 1],
            send_sem=ask_send.at[off - 1],
            recv_sem=ask_recv.at[off - 1],
            device_id={"site": site, "dom": dom_peer(off)},
            device_id_type=MESH,
        )

    for off in range(1, doms):
        ask(off).start()

    for s in site_at[1:]:
        pl.semaphore_signal(line_sem, inc=1, device_id=here(s), device_id_type=MESH)
    for off in (1, planes - 1):
        pl.semaphore_signal(next_sem, inc=1, device_id=here(plane_at[off]), device_id_type=MESH)

    row_id = lax.broadcasted_iota(jnp.int32, (ROWS, ROWS), 0)

    def entry(part):
        relative = part - me * owned
        inside = jnp.logical_and(relative >= 0, relative < owned).astype(F32)
        at = jnp.clip(relative, 0, owned - 1)
        lv = jnp.pad(left_rows[pl.ds(at, ROWS, stride=pitch), :], ((0, 0), (0, ROWS - STATES)))
        rv = jnp.pad(right_rows[pl.ds(at, ROWS, stride=pitch), :], ((0, 0), (0, ROWS - STATES)))
        pad = lambda x: jnp.pad(x, ((0, 0), (0, ROWS - STATES)))
        exponent = pad(-decay[pl.ds(at, 1), :] * rates[at])
        state_w = pad(weight[pl.ds(at, 1), :])
        lv = jnp.where(row_id == STATES, exponent, jnp.where(row_id == STATES + 1, state_w, lv))
        return jnp.concatenate([lv, rv], axis=1) * inside

    half = nblk // 2
    to_side = [dom_at[doms - 1], dom_at[1]]
    near_ids, far_ids = [0, doms - 2], 1

    def near(side, n):
        return pltpu.make_async_remote_copy(
            src_ref=near_tab.at[side, n],
            dst_ref=recv_tab.at[side, n],
            send_sem=near_send.at[side, n],
            recv_sem=near_recv.at[side, n],
            device_id={"site": site, "dom": to_side[side]},
            device_id_type=MESH,
        )

    def far(side, i):
        return pltpu.make_async_remote_copy(
            src_ref=far_tab.at[side, i],
            dst_ref=relay.at[side, i],
            send_sem=far_send.at[side, i],
            recv_sem=far_recv.at[side, i],
            device_id={"site": site, "dom": to_side[side]},
            device_id_type=MESH,
        )

    def direct(start, stop):
        @pl.loop(start, stop)
        def _(i):
            for side in range(2):
                n = (1 - side) * half + i
                near_tab[side, n] = entry(asked[near_ids[side], 0, n])
            for side in range(2):
                near(side, (1 - side) * half + i).start()

    def split(ref, out):
        @pl.loop(0, nblk)
        def _(n):
            for b in range(BR):
                hi, lo = hi_lo(ref[pl.ds(b * (STATES * nblk) + n, ROWS, stride=nblk), :])
                lanes = pl.ds((b % 2) * BLK, BLK)
                out[n, b // 2, pl.ds(0, ROWS), lanes] = hi
                out[n, b // 2, pl.ds(ROWS, ROWS), lanes] = lo

    def passed_on(start, stop):
        @pl.loop(start, stop)
        def _(i):
            for side in range(2):
                n = side * half + i
                mine = entry(asked[near_ids[side], 0, n])
                far(side, i).wait_recv()
                near_tab[side, n] = mine + relay[side, i]
            for side in range(2):
                near(side, side * half + i).start()

    for load in loads[:4] + small[1:]:
        load.wait()
    loads[4].wait()
    loads[5].wait()
    split(top, top_s)
    for off in range(1, doms):
        ask(off).wait_recv()

    @pl.loop(0, half)
    def _(i):
        for side in range(2):
            far_tab[side, i] = entry(asked[far_ids, 0, side * half + i])
        for side in range(2):
            far(side, i).start()

    direct(0, half - 2)

    @pl.loop(0, nblk)
    def _(n):
        own_tab[n] = entry(blocks[0, n])

    loads[6].wait()
    split(bottom, bottom_s)
    passed_on(0, 1)
    direct(half - 2, half - 1)
    passed_on(1, 2)
    direct(half - 1, half)
    passed_on(2, half)

    pl.semaphore_wait(next_sem, 2)
    for off in (2, planes - 2):
        pl.semaphore_signal(after_sem, inc=1, device_id=here(plane_at[off]), device_id_type=MESH)

    lane1 = lax.broadcasted_iota(jnp.int32, (1, BLK), 1)
    times = jnp.zeros((1, BLK), F32)
    for b in range(BR):
        times = jnp.where(lane1 == b, lengths[chosen[b]], times)
    lane64 = lax.broadcasted_iota(jnp.int32, (ROWS, ROWS), 1)

    @pl.loop(0, nblk)
    def _(turn):
        n = (turn % 2) * half + turn // 2
        got = own_tab[n]
        for side in range(2):
            near(side, n).wait_recv()
            got = got + recv_tab[side, n]
        lv_t = jnp.transpose(got[:, :ROWS])
        state_w = got[STATES + 1 : STATES + 2, :ROWS]
        exponent = lv_t[:, STATES : STATES + 1]
        lv_t = jnp.where(lane64 < STATES, lv_t * state_w, 0.0)
        lv_hi, lv_lo = hi_lo(lv_t)
        rv_hi, rv_lo = hi_lo(got[:, ROWS:])
        lhs_l = jnp.concatenate([lv_hi, lv_hi, lv_lo], axis=1)
        lhs_r = jnp.concatenate([rv_hi, rv_hi, rv_lo], axis=1)
        expo_b = jnp.broadcast_to(exponent, (ROWS, BLK))
        decays = jnp.exp(exponent * times)

        def stacked(ref, pair):
            x = ref[n, pair]
            return jnp.concatenate([x, x[:ROWS]], axis=0)

        for b in range(0, BR, 2):
            x, y = stacked(top_s, b // 2), stacked(bottom_s, b // 2)
            joint = dot(lhs_l, x, ((1,), (0,))) * dot(lhs_r, y, ((1,), (0,)))
            for c in range(2):
                decayed = joint[:, c * BLK : (c + 1) * BLK] * decays[:, b + c : b + c + 1]
                for power in range(3):
                    likes[power, pl.ds(b + c, 1), :] = jnp.sum(decayed, axis=0, keepdims=True)
                    if power < 2:
                        decayed = decayed * expo_b
        like0 = likes[0]
        first = likes[1] / like0
        second = likes[2] / like0 - first * first
        sites_w = pattern[pl.ds(n, 1), :].astype(F32)
        loglik_v[pl.ds(n, BR, stride=nblk), :] = sites_w * jnp.log(like0)
        sums[pl.ds(n * 32, BR), :] = sites_w * first
        sums[pl.ds(n * 32 + BR, BR), :] = sites_w * second

    stores = [
        pltpu.make_async_copy(loglik_v, loglik_out, local_sem.at[12]),
        pltpu.make_async_copy(part_v, part_out, local_sem.at[13]),
        pltpu.make_async_copy(new_v, lengths_out, local_sem.at[14]),
    ]
    stores[0].start()
    pl.semaphore_wait(line_sem, across - 1)
    pl.semaphore_wait(after_sem, 2)

    ones = jnp.ones((8, BLK), BF16)
    total = sum(dot(ones, piece, ((1,), (1,))) for piece in three(sums[...]))
    lane_blk = lax.broadcasted_iota(jnp.int32, (1, BLK), 1) // 32
    for g in range(2):
        gath[rank, pl.ds(g, 1), :] = total[0:1, g * BLK : (g + 1) * BLK]
        ids = jnp.zeros((1, BLK), F32)
        for k in range(4):
            ids = jnp.where(lane_blk == k, blocks[0, g * 4 + k].astype(F32), ids)
        gath[rank, pl.ds(2 + g, 1), :] = ids

    def give(off):
        return pltpu.make_async_remote_copy(
            src_ref=gath.at[rank],
            dst_ref=gath.at[rank],
            send_sem=gath_send.at[off],
            recv_sem=gath_recv.at[off],
            device_id=group_peer(off),
            device_id_type=MESH,
        )

    hops = lambda off, count: min(off, count - off)
    spread_out = sorted(
        range(1, group),
        key=lambda off: -hops(off // doms // 2, across // 2) - hops(off % doms, doms),
    )
    for off in spread_out:
        give(off).start()

    for off in range(1, group):
        give(off).wait_recv()

    vals = jnp.concatenate([gath[:, 0, :], gath[:, 1, :]], axis=0)
    ids = jnp.concatenate([gath[:, 2, :], gath[:, 3, :]], axis=0)
    local = lax.broadcasted_iota(jnp.int32, (2 * group, BLK), 1)
    mine = jnp.where(local < owned, local + me * owned, -1).astype(F32)
    hot = jnp.concatenate(
        [(ids[:, k * 32 : k * 32 + 1] == mine).astype(F32).astype(BF16) for k in range(4)], axis=1
    )
    vals_t = jnp.transpose(vals)
    spread = dot(
        jnp.concatenate(three(vals_t), axis=1),
        jnp.concatenate([hot, hot, hot], axis=0),
        ((1,), (0,)),
    )
    by_part = sum(spread[k * 32 : (k + 1) * 32, k * BLK : (k + 1) * BLK] for k in range(4))
    lane = lax.broadcasted_iota(jnp.int32, (BR, BLK), 1)
    zsum[plane, 0:BR, :] = jnp.where(
        lane < owned, by_part[:BR], pltpu.roll(by_part[BR:], owned, 1)
    )
    column_sum = jnp.sum(vals, axis=0, keepdims=True)
    all_sum = column_sum
    for k in range(1, 4):
        all_sum = all_sum + pltpu.roll(column_sum, 32 * k, 1)
    zsum[plane, BR : BR + 8, :] = jnp.broadcast_to(all_sum, (8, BLK))

    def pass_on(off):
        return pltpu.make_async_remote_copy(
            src_ref=zsum.at[plane],
            dst_ref=zsum.at[plane],
            send_sem=zsum_send.at[off],
            recv_sem=zsum_recv.at[off],
            device_id=plane_peer(off),
            device_id_type=MESH,
        )

    for off in sorted(range(1, planes), key=lambda off: -hops(off, planes)):
        pass_on(off).start()

    for off in range(1, planes):
        pass_on(off).wait_recv()

    done = jnp.sum(zsum[...], axis=0)
    both = done[:BR]
    part_v[0] = both[:, :owned]
    part_v[1] = pltpu.roll(both, owned, 1)[:, :owned]
    stores[1].start()
    totals = done[BR : BR + 8]
    updated = times - totals / pltpu.roll(totals, BLK - BR, 1)
    tree = lengths_v.shape[0]
    index = lax.broadcasted_iota(jnp.int32, (1, BLK), 1)
    spots = [jnp.broadcast_to(updated[0:1, b : b + 1], (1, BLK)) for b in range(BR)]
    for start in range(0, tree, BLK):
        width = min(BLK, tree - start)
        new = lengths_v[pl.ds(start, width)].reshape(1, width)
        for b in range(BR):
            new = jnp.where(index[:, :width] + start == chosen[b], spots[b][:, :width], new)
        new_v[pl.ds(start, width)] = new.reshape(width)

    stores[2].start()
    for off in range(1, doms):
        ask(off).wait_send()

    @pl.loop(0, nblk)
    def _(n):
        for side in range(2):
            near(side, n).wait_send()

    @pl.loop(0, half)
    def _(i):
        for side in range(2):
            far(side, i).wait_send()

    for off in range(1, group):
        give(off).wait_send()

    for off in range(1, planes):
        pass_on(off).wait_send()
    for store in stores:
        store.wait()


def store_kernel(loglik, share, lengths, loglik_out, share_out, lengths_out, sem):
    copies = [
        pltpu.make_async_copy(loglik, loglik_out, sem.at[0]),
        pltpu.make_async_copy(share, share_out, sem.at[1]),
        pltpu.make_async_copy(lengths, lengths_out, sem.at[2]),
    ]
    for copy in copies:
        copy.start()
    for copy in copies:
        copy.wait()


def on_device(
    sizes,
    top_partial,
    bottom_partial,
    left_vectors,
    right_vectors,
    decay_rates,
    state_weights,
    part_rates,
    branch_lengths,
    pattern_weights,
    block_partition,
    chosen_branches,
):
    planes, across, doms, nblk, owned = sizes
    flat = BR * STATES * nblk
    group = across * doms
    hbm = pl.BlockSpec(memory_space=pltpu.HBM)
    tree = branch_lengths.shape[0]
    loglik, share, lengths = pl.pallas_call(
        functools.partial(step_kernel, sizes),
        out_shape=(
            jax.ShapeDtypeStruct((BR * nblk, BLK), F32),
            jax.ShapeDtypeStruct((2, BR, owned), F32),
            jax.ShapeDtypeStruct((tree,), F32),
        ),
        in_specs=[hbm] * 11,
        out_specs=(hbm, hbm, hbm),
        scratch_shapes=[
            pltpu.VMEM((BR * nblk, BLK), F32),
            pltpu.VMEM((2, BR, owned), F32),
            pltpu.VMEM((tree,), F32),
            pltpu.VMEM((flat + (ROWS - STATES) * nblk, BLK), F32),
            pltpu.VMEM((flat + (ROWS - STATES) * nblk, BLK), F32),
            pltpu.VMEM((nblk, BR // 2, 2 * ROWS, 2 * BLK), BF16),
            pltpu.VMEM((nblk, BR // 2, 2 * ROWS, 2 * BLK), BF16),
            pltpu.VMEM((nblk, ROWS, BLK), F32),
            pltpu.VMEM((ROWS, owned + 8, STATES), F32),
            pltpu.VMEM((ROWS, owned + 8, STATES), F32),
            pltpu.VMEM((owned, STATES), F32),
            pltpu.VMEM((owned, STATES), F32),
            pltpu.VMEM((nblk, BLK), jnp.int32),
            pltpu.SMEM((owned,), F32),
            pltpu.SMEM((tree,), F32),
            pltpu.SMEM((BR,), jnp.int32),
            pltpu.SMEM((1, nblk), jnp.int32),
            pltpu.VMEM((tree,), F32),
            pltpu.SMEM((doms - 1, 1, nblk), jnp.int32),
            pltpu.VMEM((2, nblk, ROWS, BLK), F32),
            pltpu.VMEM((2, nblk // 2, ROWS, BLK), F32),
            pltpu.VMEM((2, nblk, ROWS, BLK), F32),
            pltpu.VMEM((2, nblk // 2, ROWS, BLK), F32),
            pltpu.VMEM((3, BR, BLK), F32),
            pltpu.VMEM((32 * nblk, BLK), F32),
            pltpu.VMEM((group, 4, BLK), F32),
            pltpu.VMEM((planes, BR + 8, BLK), F32),
            pltpu.SemaphoreType.DMA((15,)),
            pltpu.SemaphoreType.DMA((doms - 1,)),
            pltpu.SemaphoreType.DMA((doms - 1,)),
            pltpu.SemaphoreType.DMA((2, nblk)),
            pltpu.SemaphoreType.DMA((2, nblk)),
            pltpu.SemaphoreType.DMA((2, nblk // 2)),
            pltpu.SemaphoreType.DMA((2, nblk // 2)),
            pltpu.SemaphoreType.DMA((group,)),
            pltpu.SemaphoreType.DMA((group,)),
            pltpu.SemaphoreType.DMA((planes,)),
            pltpu.SemaphoreType.DMA((planes,)),
            pltpu.SemaphoreType.REGULAR,
            pltpu.SemaphoreType.REGULAR,
            pltpu.SemaphoreType.REGULAR,
        ],
        compiler_params=pltpu.CompilerParams(
            collective_id=0, has_side_effects=True
        ),
    )(
        top_partial.reshape(BR, STATES, nblk, BLK).reshape(flat, BLK),
        bottom_partial.reshape(BR, STATES, nblk, BLK).reshape(flat, BLK),
        jnp.transpose(left_vectors, (1, 0, 2)),
        jnp.transpose(right_vectors, (1, 0, 2)),
        decay_rates,
        state_weights,
        part_rates,
        branch_lengths,
        chosen_branches,
        block_partition,
        pattern_weights.reshape(nblk, BLK),
    )
    loglik, share, new_lengths = pl.pallas_call(
        store_kernel,
        out_shape=(
            jax.ShapeDtypeStruct((BR * nblk, BLK), F32),
            jax.ShapeDtypeStruct((2, BR, owned), F32),
            jax.ShapeDtypeStruct((tree,), F32),
        ),
        in_specs=[pl.BlockSpec(memory_space=pltpu.VMEM)] * 3,
        out_specs=(hbm, hbm, hbm),
        scratch_shapes=[pltpu.SemaphoreType.DMA((3,))],
    )(loglik, share, lengths)
    return (loglik.reshape(BR, 1, nblk * BLK), share, new_lengths)


def solution(mesh):
    sites, doms = mesh.shape["site"], mesh.shape["dom"]
    across = 8 if sites % 8 == 0 and sites > 8 else 2
    sizes = (sites // across, across, doms, 8, 256 // doms)
    return jax.shard_map(
        functools.partial(on_device, sizes),
        mesh=mesh,
        in_specs=(
            P(None, None, "dom", "site"),
            P(None, None, "dom", "site"),
            P("dom", None, None),
            P("dom", None, None),
            P("dom", None),
            P("dom", None),
            P("dom"),
            P(),
            P("dom", "site"),
            P("dom", "site"),
            P(),
        ),
        out_specs=(P(None, "dom", "site"), P(None, None, "dom"), P()),
        check_vma=False,
    )
```

```python
import functools

import jax
import jax.numpy as jnp
from jax import lax
from jax.experimental import pallas as pl
from jax.experimental.pallas import tpu as pltpu
from jax.sharding import PartitionSpec as P

BLK = 128
STATES = 61
ROWS = 64
BR = 16
F32 = jnp.float32
BF16 = jnp.bfloat16
MESH = pl.DeviceIdType.MESH


def hi_lo(x):
    hi = x.astype(BF16)
    return hi, (x - hi.astype(F32)).astype(BF16)


def three(x):
    hi = x.astype(BF16)
    rest = x - hi.astype(F32)
    mid = rest.astype(BF16)
    return hi, mid, (rest - mid.astype(F32)).astype(BF16)


def dot(a, b, contract):
    return lax.dot_general(a, b, ((contract[0], contract[1]), ((), ())), preferred_element_type=F32)


def step_kernel(
    sizes,
    top_hbm,
    bottom_hbm,
    left_hbm,
    right_hbm,
    decay_hbm,
    weight_hbm,
    rates_hbm,
    lengths_hbm,
    chosen_hbm,
    blocks_hbm,
    pattern_hbm,
    loglik_out,
    part_out,
    lengths_out,
    loglik_v,
    part_v,
    new_v,
    top,
    bottom,
    top_s,
    bottom_s,
    own_tab,
    left,
    right,
    decay,
    weight,
    pattern,
    rates,
    lengths,
    chosen,
    blocks,
    lengths_v,
    asked,
    near_tab,
    far_tab,
    recv_tab,
    relay,
    likes,
    sums,
    gath,
    zsum,
    local_sem,
    ask_send,
    ask_recv,
    near_send,
    near_recv,
    far_send,
    far_recv,
    gath_send,
    gath_recv,
    zsum_send,
    zsum_recv,
    line_sem,
    next_sem,
    after_sem,
):
    planes, across, doms, nblk, owned = sizes
    site = lax.axis_index("site")
    me = lax.axis_index("dom")
    plane = site // across
    column = site % across
    group = across * doms
    rank = column * doms + me
    def wait_for(ref, sem):
        pltpu.make_async_copy(ref, ref, sem).wait()

    dom_at = [me] + [lax.rem(me + off, doms) for off in range(1, doms)]
    dom_peer = lambda off: dom_at[off]
    site_at = [site] + [plane * across + lax.rem(column + off, across) for off in range(1, across)]
    plane_at = [site] + [lax.rem(plane + off, planes) * across + column for off in range(1, planes)]

    def group_peer(off):
        return {"site": site_at[off // doms], "dom": dom_at[off % doms]}

    def plane_peer(off):
        return {"site": plane_at[off], "dom": me}

    small = [
        pltpu.make_async_copy(blocks_hbm, blocks, local_sem.at[7]),
        pltpu.make_async_copy(rates_hbm, rates, local_sem.at[8]),
        pltpu.make_async_copy(chosen_hbm, chosen, local_sem.at[9]),
        pltpu.make_async_copy(lengths_hbm, lengths, local_sem.at[10]),
    ]
    small.append(pltpu.make_async_copy(lengths_hbm, lengths_v, local_sem.at[11]))
    small[0].start()
    loads = [
        pltpu.make_async_copy(left_hbm, left.at[pl.ds(0, STATES), pl.ds(0, owned)], local_sem.at[0]),
        pltpu.make_async_copy(right_hbm, right.at[pl.ds(0, STATES), pl.ds(0, owned)], local_sem.at[1]),
        pltpu.make_async_copy(decay_hbm, decay, local_sem.at[2]),
        pltpu.make_async_copy(weight_hbm, weight, local_sem.at[3]),
        pltpu.make_async_copy(pattern_hbm, pattern, local_sem.at[4]),
        pltpu.make_async_copy(top_hbm, top.at[pl.ds(0, BR * STATES * nblk)], local_sem.at[5]),
        pltpu.make_async_copy(bottom_hbm, bottom.at[pl.ds(0, BR * STATES * nblk)], local_sem.at[6]),
    ]
    for load in loads[:4] + small[1:] + loads[4:]:
        load.start()

    barrier = pltpu.get_barrier_semaphore()
    here = lambda s: {"site": s, "dom": me}
    near = [{"site": site, "dom": d} for d in dom_at[1:]]
    near += [here(s) for s in site_at[1:]] + [here(plane_at[1]), here(plane_at[planes - 1])]
    for device in near:
        pl.semaphore_signal(barrier, inc=1, device_id=device, device_id_type=MESH)

    small[0].wait()
    pl.semaphore_wait(barrier, len(near))

    def ask(off):
        return pltpu.make_async_remote_copy(
            src_ref=blocks,
            dst_ref=asked.at[off - 1],
            send_sem=ask_send,
            recv_sem=ask_recv.at[off - 1],
            device_id={"site": site, "dom": dom_peer(off)},
            device_id_type=MESH,
        )

    for off in range(1, doms):
        ask(off).start()

    pitch = left.shape[1]
    tail = (ROWS - STATES, pitch, STATES)
    left[pl.ds(STATES, ROWS - STATES)] = jnp.zeros(tail, F32)
    right[pl.ds(STATES, ROWS - STATES)] = jnp.zeros(tail, F32)
    left_rows = left.reshape(ROWS * pitch, STATES)
    right_rows = right.reshape(ROWS * pitch, STATES)
    tail = (ROWS - STATES) * nblk
    top[pl.ds(BR * STATES * nblk, tail), :] = jnp.zeros((tail, BLK), F32)
    bottom[pl.ds(BR * STATES * nblk, tail), :] = jnp.zeros((tail, BLK), F32)

    for s in site_at[1:]:
        pl.semaphore_signal(line_sem, inc=1, device_id=here(s), device_id_type=MESH)
    for off in (1, planes - 1):
        pl.semaphore_signal(next_sem, inc=1, device_id=here(plane_at[off]), device_id_type=MESH)

    row_id = lax.broadcasted_iota(jnp.int32, (ROWS, ROWS), 0)

    def entry(part):
        relative = part - me * owned
        inside = jnp.logical_and(relative >= 0, relative < owned).astype(F32)
        at = jnp.clip(relative, 0, owned - 1)
        lv = jnp.pad(left_rows[pl.ds(at, ROWS, stride=pitch), :], ((0, 0), (0, ROWS - STATES)))
        rv = jnp.pad(right_rows[pl.ds(at, ROWS, stride=pitch), :], ((0, 0), (0, ROWS - STATES)))
        pad = lambda x: jnp.pad(x, ((0, 0), (0, ROWS - STATES)))
        exponent = pad(-decay[pl.ds(at, 1), :] * rates[at])
        state_w = pad(weight[pl.ds(at, 1), :])
        lv = jnp.where(row_id == STATES, exponent, jnp.where(row_id == STATES + 1, state_w, lv))
        return jnp.concatenate([lv, rv], axis=1) * inside

    half = nblk // 2
    to_side = [dom_at[doms - 1], dom_at[1]]
    near_ids, far_ids = [0, doms - 2], 1

    def near(side, n):
        return pltpu.make_async_remote_copy(
            src_ref=near_tab.at[side, n],
            dst_ref=recv_tab.at[side, n],
            send_sem=near_send,
            recv_sem=near_recv.at[n],
            device_id={"site": site, "dom": to_side[side]},
            device_id_type=MESH,
        )

    def far(side, i):
        return pltpu.make_async_remote_copy(
            src_ref=far_tab.at[side, i],
            dst_ref=relay.at[side, i],
            send_sem=far_send,
            recv_sem=far_recv.at[i],
            device_id={"site": site, "dom": to_side[side]},
            device_id_type=MESH,
        )

    def direct(start, stop):
        @pl.loop(start, stop)
        def _(i):
            for side in range(2):
                n = (1 - side) * half + i
                near_tab[side, n] = entry(asked[near_ids[side], 0, n])
            for side in range(2):
                near(side, (1 - side) * half + i).start()

    def split(ref, out):
        @pl.loop(0, nblk)
        def _(n):
            for b in range(BR):
                hi, lo = hi_lo(ref[pl.ds(b * (STATES * nblk) + n, ROWS, stride=nblk), :])
                lanes = pl.ds((b % 2) * BLK, BLK)
                out[n, b // 2, pl.ds(0, ROWS), lanes] = hi
                out[n, b // 2, pl.ds(ROWS, ROWS), lanes] = lo

    def passed_on(start, stop):
        @pl.loop(start, stop)
        def _(i):
            mine = [entry(asked[near_ids[side], 0, side * half + i]) for side in range(2)]
            wait_for(relay.at[:, i], far_recv.at[i])
            for side in range(2):
                near_tab[side, side * half + i] = mine[side] + relay[side, i]
            for side in range(2):
                near(side, side * half + i).start()

    for load in loads[:4] + small[1:]:
        load.wait()
    loads[4].wait()
    loads[5].wait()
    split(top, top_s)
    for off in range(1, doms):
        ask(off).wait_recv()

    @pl.loop(0, half)
    def _(i):
        for side in range(2):
            far_tab[side, i] = entry(asked[far_ids, 0, side * half + i])
        for side in range(2):
            far(side, i).start()

    direct(0, half - 2)

    @pl.loop(0, nblk)
    def _(n):
        own_tab[n] = entry(blocks[0, n])

    loads[6].wait()
    split(bottom, bottom_s)
    passed_on(0, 1)
    direct(half - 2, half - 1)
    passed_on(1, 2)
    direct(half - 1, half)
    passed_on(2, half)

    pl.semaphore_wait(next_sem, 2)
    for off in (2, planes - 2):
        pl.semaphore_signal(after_sem, inc=1, device_id=here(plane_at[off]), device_id_type=MESH)

    lane1 = lax.broadcasted_iota(jnp.int32, (1, BLK), 1)
    times = jnp.zeros((1, BLK), F32)
    for b in range(BR):
        times = jnp.where(lane1 == b, lengths[chosen[b]], times)
    lane64 = lax.broadcasted_iota(jnp.int32, (ROWS, ROWS), 1)

    def one_block(n, slot):
        got = own_tab[n]
        for side in range(2):
            got = got + recv_tab[side, n]
        lv_t = jnp.transpose(got[:, :ROWS])
        state_w = got[STATES + 1 : STATES + 2, :ROWS]
        exponent = lv_t[:, STATES : STATES + 1]
        lv_t = jnp.where(lane64 < STATES, lv_t * state_w, 0.0)
        lv_hi, lv_lo = hi_lo(lv_t)
        rv_hi, rv_lo = hi_lo(got[:, ROWS:])
        lhs_l = jnp.concatenate([lv_hi, lv_hi, lv_lo], axis=1)
        lhs_r = jnp.concatenate([rv_hi, rv_hi, rv_lo], axis=1)
        expo_b = jnp.broadcast_to(exponent, (ROWS, BLK))
        decays = jnp.exp(exponent * times)

        def stacked(ref, pair):
            x = ref[n, pair]
            return jnp.concatenate([x, x[:ROWS]], axis=0)

        for b in range(0, BR, 2):
            x, y = stacked(top_s, b // 2), stacked(bottom_s, b // 2)
            joint = dot(lhs_l, x, ((1,), (0,))) * dot(lhs_r, y, ((1,), (0,)))
            for c in range(2):
                decayed = joint[:, c * BLK : (c + 1) * BLK] * decays[:, b + c : b + c + 1]
                for power in range(3):
                    likes[slot, power, pl.ds(b + c, 1), :] = jnp.sum(decayed, axis=0, keepdims=True)
                    if power < 2:
                        decayed = decayed * expo_b
        like0, like1, like2 = (likes[slot, power] for power in range(3))
        first = like1 / like0
        second = like2 / like0 - first * first
        sites_w = pattern[pl.ds(n, 1), :].astype(F32)
        loglik_v[pl.ds(n, BR, stride=nblk), :] = sites_w * jnp.log(like0)
        sums[pl.ds(n * 32, BR), :] = sites_w * first
        sums[pl.ds(n * 32 + BR, BR), :] = sites_w * second

    @pl.loop(0, half)
    def _(i):
        for side in range(2):
            wait_for(recv_tab.at[:, side * half + i], near_recv.at[side * half + i])
        for side in range(2):
            one_block(side * half + i, side)

    stores = [
        pltpu.make_async_copy(loglik_v, loglik_out, local_sem.at[12]),
        pltpu.make_async_copy(part_v, part_out, local_sem.at[13]),
        pltpu.make_async_copy(new_v, lengths_out, local_sem.at[14]),
    ]
    stores[0].start()
    pl.semaphore_wait(line_sem, across - 1)
    pl.semaphore_wait(after_sem, 2)

    ones = jnp.ones((8, BLK), BF16)
    total = sum(dot(ones, piece, ((1,), (1,))) for piece in three(sums[...]))
    lane_blk = lax.broadcasted_iota(jnp.int32, (1, BLK), 1) // 32
    for g in range(2):
        gath[rank, pl.ds(g, 1), :] = total[0:1, g * BLK : (g + 1) * BLK]
        ids = jnp.zeros((1, BLK), F32)
        for k in range(4):
            ids = jnp.where(lane_blk == k, blocks[0, g * 4 + k].astype(F32), ids)
        gath[rank, pl.ds(2 + g, 1), :] = ids

    def give(off):
        return pltpu.make_async_remote_copy(
            src_ref=gath.at[rank],
            dst_ref=gath.at[rank],
            send_sem=gath_send,
            recv_sem=gath_recv,
            device_id=group_peer(off),
            device_id_type=MESH,
        )

    hops = lambda off, count: min(off, count - off)
    spread_out = sorted(
        range(1, group),
        key=lambda off: -hops(off // doms // 2, across // 2) - hops(off % doms, doms),
    )
    for off in spread_out:
        give(off).start()

    wait_for(gath.at[pl.ds(0, group - 1)], gath_recv)

    vals = jnp.concatenate([gath[:, 0, :], gath[:, 1, :]], axis=0)
    ids = jnp.concatenate([gath[:, 2, :], gath[:, 3, :]], axis=0)
    local = lax.broadcasted_iota(jnp.int32, (2 * group, BLK), 1)
    mine = jnp.where(local < owned, local + me * owned, -1).astype(F32)
    hot = jnp.concatenate(
        [(ids[:, k * 32 : k * 32 + 1] == mine).astype(F32).astype(BF16) for k in range(4)], axis=1
    )
    vals_t = jnp.transpose(vals)
    spread = dot(
        jnp.concatenate(three(vals_t), axis=1),
        jnp.concatenate([hot, hot, hot], axis=0),
        ((1,), (0,)),
    )
    by_part = sum(spread[k * 32 : (k + 1) * 32, k * BLK : (k + 1) * BLK] for k in range(4))
    lane = lax.broadcasted_iota(jnp.int32, (BR, BLK), 1)
    zsum[plane, 0:BR, :] = jnp.where(
        lane < owned, by_part[:BR], pltpu.roll(by_part[BR:], owned, 1)
    )
    column_sum = jnp.sum(vals, axis=0, keepdims=True)
    all_sum = column_sum
    for k in range(1, 4):
        all_sum = all_sum + pltpu.roll(column_sum, 32 * k, 1)
    zsum[plane, BR : BR + 1, :] = all_sum

    def pass_on(off):
        return pltpu.make_async_remote_copy(
            src_ref=zsum.at[plane],
            dst_ref=zsum.at[plane],
            send_sem=zsum_send,
            recv_sem=zsum_recv,
            device_id=plane_peer(off),
            device_id_type=MESH,
        )

    for off in sorted(range(1, planes), key=lambda off: -hops(off, planes)):
        pass_on(off).start()

    wait_for(zsum.at[pl.ds(0, planes - 1)], zsum_recv)

    done = jnp.sum(zsum[...], axis=0)
    both = done[:BR]
    part_v[0] = both[:, :owned]
    part_v[1] = pltpu.roll(both, owned, 1)[:, :owned]
    stores[1].start()
    totals = jnp.broadcast_to(done[BR : BR + 1], (8, BLK))
    updated = times - totals / pltpu.roll(totals, BLK - BR, 1)
    tree = lengths_v.shape[0]
    index = lax.broadcasted_iota(jnp.int32, (1, BLK), 1)
    spots = [jnp.broadcast_to(updated[0:1, b : b + 1], (1, BLK)) for b in range(BR)]
    for start in range(0, tree, BLK):
        width = min(BLK, tree - start)
        new = lengths_v[pl.ds(start, width)].reshape(1, width)
        for b in range(BR):
            new = jnp.where(index[:, :width] + start == chosen[b], spots[b][:, :width], new)
        new_v[pl.ds(start, width)] = new.reshape(width)

    stores[2].start()
    wait_for(asked, ask_send)
    wait_for(near_tab, near_send)
    wait_for(far_tab, far_send)
    wait_for(gath.at[pl.ds(0, group - 1)], gath_send)
    wait_for(zsum.at[pl.ds(0, planes - 1)], zsum_send)
    for store in stores:
        store.wait()


def store_kernel(loglik, share, lengths, loglik_out, share_out, lengths_out, sem):
    copies = [
        pltpu.make_async_copy(loglik, loglik_out, sem.at[0]),
        pltpu.make_async_copy(share, share_out, sem.at[1]),
        pltpu.make_async_copy(lengths, lengths_out, sem.at[2]),
    ]
    for copy in copies:
        copy.start()
    for copy in copies:
        copy.wait()


def on_device(
    sizes,
    top_partial,
    bottom_partial,
    left_vectors,
    right_vectors,
    decay_rates,
    state_weights,
    part_rates,
    branch_lengths,
    pattern_weights,
    block_partition,
    chosen_branches,
):
    planes, across, doms, nblk, owned = sizes
    flat = BR * STATES * nblk
    group = across * doms
    hbm = pl.BlockSpec(memory_space=pltpu.HBM)
    tree = branch_lengths.shape[0]
    loglik, share, lengths = pl.pallas_call(
        functools.partial(step_kernel, sizes),
        out_shape=(
            jax.ShapeDtypeStruct((BR * nblk, BLK), F32),
            jax.ShapeDtypeStruct((2, BR, owned), F32),
            jax.ShapeDtypeStruct((tree,), F32),
        ),
        in_specs=[hbm] * 11,
        out_specs=(hbm, hbm, hbm),
        scratch_shapes=[
            pltpu.VMEM((BR * nblk, BLK), F32),
            pltpu.VMEM((2, BR, owned), F32),
            pltpu.VMEM((tree,), F32),
            pltpu.VMEM((flat + (ROWS - STATES) * nblk, BLK), F32),
            pltpu.VMEM((flat + (ROWS - STATES) * nblk, BLK), F32),
            pltpu.VMEM((nblk, BR // 2, 2 * ROWS, 2 * BLK), BF16),
            pltpu.VMEM((nblk, BR // 2, 2 * ROWS, 2 * BLK), BF16),
            pltpu.VMEM((nblk, ROWS, BLK), F32),
            pltpu.VMEM((ROWS, owned + 8, STATES), F32),
            pltpu.VMEM((ROWS, owned + 8, STATES), F32),
            pltpu.VMEM((owned, STATES), F32),
            pltpu.VMEM((owned, STATES), F32),
            pltpu.VMEM((nblk, BLK), jnp.int32),
            pltpu.SMEM((owned,), F32),
            pltpu.SMEM((tree,), F32),
            pltpu.SMEM((BR,), jnp.int32),
            pltpu.SMEM((1, nblk), jnp.int32),
            pltpu.VMEM((tree,), F32),
            pltpu.SMEM((doms - 1, 1, nblk), jnp.int32),
            pltpu.VMEM((2, nblk, ROWS, BLK), F32),
            pltpu.VMEM((2, nblk // 2, ROWS, BLK), F32),
            pltpu.VMEM((2, nblk, ROWS, BLK), F32),
            pltpu.VMEM((2, nblk // 2, ROWS, BLK), F32),
            pltpu.VMEM((2, 3, BR, BLK), F32),
            pltpu.VMEM((32 * nblk, BLK), F32),
            pltpu.VMEM((group, 4, BLK), F32),
            pltpu.VMEM((planes, BR + 1, BLK), F32),
            pltpu.SemaphoreType.DMA((15,)),
            pltpu.SemaphoreType.DMA,
            pltpu.SemaphoreType.DMA((doms - 1,)),
            pltpu.SemaphoreType.DMA,
            pltpu.SemaphoreType.DMA((nblk,)),
            pltpu.SemaphoreType.DMA,
            pltpu.SemaphoreType.DMA((nblk // 2,)),
            pltpu.SemaphoreType.DMA,
            pltpu.SemaphoreType.DMA,
            pltpu.SemaphoreType.DMA,
            pltpu.SemaphoreType.DMA,
            pltpu.SemaphoreType.REGULAR,
            pltpu.SemaphoreType.REGULAR,
            pltpu.SemaphoreType.REGULAR,
        ],
        compiler_params=pltpu.CompilerParams(
            collective_id=0, has_side_effects=True
        ),
    )(
        top_partial.reshape(BR, STATES, nblk, BLK).reshape(flat, BLK),
        bottom_partial.reshape(BR, STATES, nblk, BLK).reshape(flat, BLK),
        jnp.transpose(left_vectors, (1, 0, 2)),
        jnp.transpose(right_vectors, (1, 0, 2)),
        decay_rates,
        state_weights,
        part_rates,
        branch_lengths,
        chosen_branches,
        block_partition,
        pattern_weights.reshape(nblk, BLK),
    )
    loglik, share, new_lengths = pl.pallas_call(
        store_kernel,
        out_shape=(
            jax.ShapeDtypeStruct((BR * nblk, BLK), F32),
            jax.ShapeDtypeStruct((2, BR, owned), F32),
            jax.ShapeDtypeStruct((tree,), F32),
        ),
        in_specs=[pl.BlockSpec(memory_space=pltpu.VMEM)] * 3,
        out_specs=(hbm, hbm, hbm),
        scratch_shapes=[pltpu.SemaphoreType.DMA((3,))],
    )(loglik, share, lengths)
    return (loglik.reshape(BR, 1, nblk * BLK), share, new_lengths)


def solution(mesh):
    sites, doms = mesh.shape["site"], mesh.shape["dom"]
    across = 8 if sites % 8 == 0 and sites > 8 else 2
    sizes = (sites // across, across, doms, 8, 256 // doms)
    return jax.shard_map(
        functools.partial(on_device, sizes),
        mesh=mesh,
        in_specs=(
            P(None, None, "dom", "site"),
            P(None, None, "dom", "site"),
            P("dom", None, None),
            P("dom", None, None),
            P("dom", None),
            P("dom", None),
            P("dom"),
            P(),
            P("dom", "site"),
            P("dom", "site"),
            P(),
        ),
        out_specs=(P(None, "dom", "site"), P(None, None, "dom"), P()),
        check_vma=False,
    )
```

```python
import functools

import jax
import jax.numpy as jnp
from jax import lax
from jax.experimental import pallas as pl
from jax.experimental.pallas import tpu as pltpu
from jax.sharding import PartitionSpec as P

BLK = 128
STATES = 61
ROWS = 64
BR = 16
F32 = jnp.float32
BF16 = jnp.bfloat16
MESH = pl.DeviceIdType.MESH


def hi_lo(x):
    hi = x.astype(BF16)
    return hi, (x - hi.astype(F32)).astype(BF16)


def three(x):
    hi = x.astype(BF16)
    rest = x - hi.astype(F32)
    mid = rest.astype(BF16)
    return hi, mid, (rest - mid.astype(F32)).astype(BF16)


def dot(a, b, contract):
    return lax.dot_general(a, b, ((contract[0], contract[1]), ((), ())), preferred_element_type=F32)


def step_kernel(
    sizes,
    top_hbm,
    bottom_hbm,
    left_hbm,
    right_hbm,
    decay_hbm,
    weight_hbm,
    rates_hbm,
    lengths_hbm,
    chosen_hbm,
    blocks_hbm,
    pattern_hbm,
    loglik_out,
    part_out,
    lengths_out,
    top,
    bottom,
    top_s,
    bottom_s,
    own_tab,
    left,
    right,
    decay,
    weight,
    pattern,
    rates,
    lengths,
    chosen,
    blocks,
    lengths_v,
    asked,
    near_tab,
    far_tab,
    recv_tab,
    relay,
    likes,
    sums,
    gath,
    zsum,
    local_sem,
    ask_send,
    ask_recv,
    near_send,
    near_recv,
    far_send,
    far_recv,
    gath_send,
    gath_recv,
    zsum_send,
    zsum_recv,
    line_sem,
    next_sem,
    after_sem,
):
    planes, across, doms, nblk, owned = sizes
    site = lax.axis_index("site")
    me = lax.axis_index("dom")
    plane = site // across
    column = site % across
    group = across * doms
    rank = column * doms + me
    def wait_for(ref, sem):
        pltpu.make_async_copy(ref, ref, sem).wait()

    dom_at = [me] + [lax.rem(me + off, doms) for off in range(1, doms)]
    dom_peer = lambda off: dom_at[off]
    site_at = [site] + [plane * across + lax.rem(column + off, across) for off in range(1, across)]
    plane_at = [site] + [lax.rem(plane + off, planes) * across + column for off in range(1, planes)]

    def group_peer(off):
        return {"site": site_at[off // doms], "dom": dom_at[off % doms]}

    def plane_peer(off):
        return {"site": plane_at[off], "dom": me}

    small = [
        pltpu.make_async_copy(blocks_hbm, blocks, local_sem.at[7]),
        pltpu.make_async_copy(rates_hbm, rates, local_sem.at[8]),
        pltpu.make_async_copy(chosen_hbm, chosen, local_sem.at[9]),
        pltpu.make_async_copy(lengths_hbm, lengths, local_sem.at[10]),
    ]
    small.append(pltpu.make_async_copy(lengths_hbm, lengths_v, local_sem.at[11]))
    small[0].start()
    loads = [
        pltpu.make_async_copy(left_hbm, left.at[pl.ds(0, STATES), pl.ds(0, owned)], local_sem.at[0]),
        pltpu.make_async_copy(right_hbm, right.at[pl.ds(0, STATES), pl.ds(0, owned)], local_sem.at[1]),
        pltpu.make_async_copy(decay_hbm, decay, local_sem.at[2]),
        pltpu.make_async_copy(weight_hbm, weight, local_sem.at[3]),
        pltpu.make_async_copy(pattern_hbm, pattern, local_sem.at[4]),
        pltpu.make_async_copy(top_hbm, top.at[pl.ds(0, BR * STATES * nblk)], local_sem.at[5]),
        pltpu.make_async_copy(bottom_hbm, bottom.at[pl.ds(0, BR * STATES * nblk)], local_sem.at[6]),
    ]
    for load in loads[:4] + small[1:] + loads[4:]:
        load.start()

    barrier = pltpu.get_barrier_semaphore()
    here = lambda s: {"site": s, "dom": me}
    near = [{"site": site, "dom": d} for d in dom_at[1:]]
    near += [here(s) for s in site_at[1:]] + [here(plane_at[1]), here(plane_at[planes - 1])]
    for device in near:
        pl.semaphore_signal(barrier, inc=1, device_id=device, device_id_type=MESH)

    small[0].wait()
    pl.semaphore_wait(barrier, len(near))

    def ask(off):
        return pltpu.make_async_remote_copy(
            src_ref=blocks,
            dst_ref=asked.at[off - 1],
            send_sem=ask_send,
            recv_sem=ask_recv.at[off - 1],
            device_id={"site": site, "dom": dom_peer(off)},
            device_id_type=MESH,
        )

    for off in range(1, doms):
        ask(off).start()

    pitch = left.shape[1]
    tail = (ROWS - STATES, pitch, STATES)
    left[pl.ds(STATES, ROWS - STATES)] = jnp.zeros(tail, F32)
    right[pl.ds(STATES, ROWS - STATES)] = jnp.zeros(tail, F32)
    left_rows = left.reshape(ROWS * pitch, STATES)
    right_rows = right.reshape(ROWS * pitch, STATES)
    tail = (ROWS - STATES) * nblk
    top[pl.ds(BR * STATES * nblk, tail), :] = jnp.zeros((tail, BLK), F32)
    bottom[pl.ds(BR * STATES * nblk, tail), :] = jnp.zeros((tail, BLK), F32)

    for s in site_at[1:]:
        pl.semaphore_signal(line_sem, inc=1, device_id=here(s), device_id_type=MESH)
    for off in (1, planes - 1):
        pl.semaphore_signal(next_sem, inc=1, device_id=here(plane_at[off]), device_id_type=MESH)

    row_id = lax.broadcasted_iota(jnp.int32, (ROWS, ROWS), 0)

    def entry(part):
        relative = part - me * owned
        inside = jnp.logical_and(relative >= 0, relative < owned).astype(F32)
        at = jnp.clip(relative, 0, owned - 1)
        lv = jnp.pad(left_rows[pl.ds(at, ROWS, stride=pitch), :], ((0, 0), (0, ROWS - STATES)))
        rv = jnp.pad(right_rows[pl.ds(at, ROWS, stride=pitch), :], ((0, 0), (0, ROWS - STATES)))
        pad = lambda x: jnp.pad(x, ((0, 0), (0, ROWS - STATES)))
        exponent = pad(-decay[pl.ds(at, 1), :] * rates[at])
        state_w = pad(weight[pl.ds(at, 1), :])
        lv = jnp.where(row_id == STATES, exponent, jnp.where(row_id == STATES + 1, state_w, lv))
        return jnp.concatenate([lv, rv], axis=1) * inside

    half = nblk // 2
    to_side = [dom_at[doms - 1], dom_at[1]]
    near_ids, far_ids = [0, doms - 2], 1

    def near(side, n):
        return pltpu.make_async_remote_copy(
            src_ref=near_tab.at[side, n],
            dst_ref=recv_tab.at[side, n],
            send_sem=near_send,
            recv_sem=near_recv.at[n],
            device_id={"site": site, "dom": to_side[side]},
            device_id_type=MESH,
        )

    def far(side, i):
        return pltpu.make_async_remote_copy(
            src_ref=far_tab.at[side, i],
            dst_ref=relay.at[side, i],
            send_sem=far_send,
            recv_sem=far_recv.at[i],
            device_id={"site": site, "dom": to_side[side]},
            device_id_type=MESH,
        )

    def direct(start, stop):
        @pl.loop(start, stop)
        def _(i):
            for side in range(2):
                n = (1 - side) * half + i
                near_tab[side, n] = entry(asked[near_ids[side], 0, n])
            for side in range(2):
                near(side, (1 - side) * half + i).start()

    def split(ref, out):
        @pl.loop(0, nblk)
        def _(n):
            for b in range(BR):
                hi, lo = hi_lo(ref[pl.ds(b * (STATES * nblk) + n, ROWS, stride=nblk), :])
                lanes = pl.ds((b % 2) * BLK, BLK)
                out[n, b // 2, pl.ds(0, ROWS), lanes] = hi
                out[n, b // 2, pl.ds(ROWS, ROWS), lanes] = lo

    def passed_on(start, stop):
        @pl.loop(start, stop)
        def _(i):
            mine = [entry(asked[near_ids[side], 0, side * half + i]) for side in range(2)]
            wait_for(relay.at[:, i], far_recv.at[i])
            for side in range(2):
                near_tab[side, side * half + i] = mine[side] + relay[side, i]
            for side in range(2):
                near(side, side * half + i).start()

    for load in loads[:4] + small[1:]:
        load.wait()
    loads[4].wait()
    loads[5].wait()
    split(top, top_s)
    for off in range(1, doms):
        ask(off).wait_recv()

    @pl.loop(0, half)
    def _(i):
        for side in range(2):
            far_tab[side, i] = entry(asked[far_ids, 0, side * half + i])
        for side in range(2):
            far(side, i).start()

    direct(0, half - 2)

    @pl.loop(0, nblk)
    def _(n):
        own_tab[n] = entry(blocks[0, n])

    loads[6].wait()
    split(bottom, bottom_s)
    passed_on(0, 1)
    direct(half - 2, half - 1)
    passed_on(1, 2)
    direct(half - 1, half)
    passed_on(2, half)

    pl.semaphore_wait(next_sem, 2)
    for off in (2, planes - 2):
        pl.semaphore_signal(after_sem, inc=1, device_id=here(plane_at[off]), device_id_type=MESH)

    lane1 = lax.broadcasted_iota(jnp.int32, (1, BLK), 1)
    times = jnp.zeros((1, BLK), F32)
    for b in range(BR):
        times = jnp.where(lane1 == b, lengths[chosen[b]], times)
    lane64 = lax.broadcasted_iota(jnp.int32, (ROWS, ROWS), 1)

    def one_block(n, slot):
        got = own_tab[n]
        for side in range(2):
            got = got + recv_tab[side, n]
        lv_t = jnp.transpose(got[:, :ROWS])
        state_w = got[STATES + 1 : STATES + 2, :ROWS]
        exponent = lv_t[:, STATES : STATES + 1]
        lv_t = jnp.where(lane64 < STATES, lv_t * state_w, 0.0)
        lv_hi, lv_lo = hi_lo(lv_t)
        rv_hi, rv_lo = hi_lo(got[:, ROWS:])
        lhs_l = jnp.concatenate([lv_hi, lv_hi, lv_lo], axis=1)
        lhs_r = jnp.concatenate([rv_hi, rv_hi, rv_lo], axis=1)
        expo_b = jnp.broadcast_to(exponent, (ROWS, BLK))
        decays = jnp.exp(exponent * times)

        def stacked(ref, pair):
            x = ref[n, pair]
            return jnp.concatenate([x, x[:ROWS]], axis=0)

        for b in range(0, BR, 2):
            x, y = stacked(top_s, b // 2), stacked(bottom_s, b // 2)
            joint = dot(lhs_l, x, ((1,), (0,))) * dot(lhs_r, y, ((1,), (0,)))
            for c in range(2):
                decayed = joint[:, c * BLK : (c + 1) * BLK] * decays[:, b + c : b + c + 1]
                for power in range(3):
                    likes[slot, power, pl.ds(b + c, 1), :] = jnp.sum(decayed, axis=0, keepdims=True)
                    if power < 2:
                        decayed = decayed * expo_b
        like0, like1, like2 = (likes[slot, power] for power in range(3))
        first = like1 / like0
        second = like2 / like0 - first * first
        sites_w = pattern[pl.ds(n, 1), :].astype(F32)
        loglik_out[pl.ds(n, BR, stride=nblk), :] = sites_w * jnp.log(like0)
        sums[pl.ds(n * 32, BR), :] = sites_w * first
        sums[pl.ds(n * 32 + BR, BR), :] = sites_w * second

    @pl.loop(0, half)
    def _(i):
        for side in range(2):
            wait_for(recv_tab.at[:, side * half + i], near_recv.at[side * half + i])
        for side in range(2):
            one_block(side * half + i, side)

    pl.semaphore_wait(line_sem, across - 1)
    pl.semaphore_wait(after_sem, 2)

    ones = jnp.ones((8, BLK), BF16)
    total = sum(dot(ones, piece, ((1,), (1,))) for piece in three(sums[...]))
    lane_blk = lax.broadcasted_iota(jnp.int32, (1, BLK), 1) // 32
    for g in range(2):
        gath[rank, pl.ds(g, 1), :] = total[0:1, g * BLK : (g + 1) * BLK]
        ids = jnp.zeros((1, BLK), F32)
        for k in range(4):
            ids = jnp.where(lane_blk == k, blocks[0, g * 4 + k].astype(F32), ids)
        gath[rank, pl.ds(2 + g, 1), :] = ids

    def give(off):
        return pltpu.make_async_remote_copy(
            src_ref=gath.at[rank],
            dst_ref=gath.at[rank],
            send_sem=gath_send,
            recv_sem=gath_recv,
            device_id=group_peer(off),
            device_id_type=MESH,
        )

    hops = lambda off, count: min(off, count - off)
    spread_out = sorted(
        range(1, group),
        key=lambda off: -hops(off // doms // 2, across // 2) - hops(off % doms, doms),
    )
    for off in spread_out:
        give(off).start()

    wait_for(gath.at[pl.ds(0, group - 1)], gath_recv)

    vals = jnp.concatenate([gath[:, 0, :], gath[:, 1, :]], axis=0)
    ids = jnp.concatenate([gath[:, 2, :], gath[:, 3, :]], axis=0)
    local = lax.broadcasted_iota(jnp.int32, (2 * group, BLK), 1)
    mine = jnp.where(local < owned, local + me * owned, -1).astype(F32)
    hot = jnp.concatenate(
        [(ids[:, k * 32 : k * 32 + 1] == mine).astype(F32).astype(BF16) for k in range(4)], axis=1
    )
    vals_t = jnp.transpose(vals)
    spread = dot(
        jnp.concatenate(three(vals_t), axis=1),
        jnp.concatenate([hot, hot, hot], axis=0),
        ((1,), (0,)),
    )
    by_part = sum(spread[k * 32 : (k + 1) * 32, k * BLK : (k + 1) * BLK] for k in range(4))
    lane = lax.broadcasted_iota(jnp.int32, (BR, BLK), 1)
    zsum[plane, 0:BR, :] = jnp.where(
        lane < owned, by_part[:BR], pltpu.roll(by_part[BR:], owned, 1)
    )
    column_sum = jnp.sum(vals, axis=0, keepdims=True)
    all_sum = column_sum
    for k in range(1, 4):
        all_sum = all_sum + pltpu.roll(column_sum, 32 * k, 1)
    zsum[plane, BR : BR + 1, :] = all_sum

    def pass_on(off):
        return pltpu.make_async_remote_copy(
            src_ref=zsum.at[plane],
            dst_ref=zsum.at[plane],
            send_sem=zsum_send,
            recv_sem=zsum_recv,
            device_id=plane_peer(off),
            device_id_type=MESH,
        )

    for off in sorted(range(1, planes), key=lambda off: -hops(off, planes)):
        pass_on(off).start()

    wait_for(zsum.at[pl.ds(0, planes - 1)], zsum_recv)

    done = jnp.sum(zsum[...], axis=0)
    both = done[:BR]
    part_out[0] = both[:, :owned]
    part_out[1] = pltpu.roll(both, owned, 1)[:, :owned]
    totals = jnp.broadcast_to(done[BR : BR + 1], (8, BLK))
    updated = times - totals / pltpu.roll(totals, BLK - BR, 1)
    tree = lengths_v.shape[0]
    index = lax.broadcasted_iota(jnp.int32, (1, BLK), 1)
    spots = [jnp.broadcast_to(updated[0:1, b : b + 1], (1, BLK)) for b in range(BR)]
    for start in range(0, tree, BLK):
        width = min(BLK, tree - start)
        new = lengths_v[pl.ds(start, width)].reshape(1, width)
        for b in range(BR):
            new = jnp.where(index[:, :width] + start == chosen[b], spots[b][:, :width], new)
        lengths_out[pl.ds(start, width)] = new.reshape(width)

    wait_for(asked, ask_send)
    wait_for(near_tab, near_send)
    wait_for(far_tab, far_send)
    wait_for(gath.at[pl.ds(0, group - 1)], gath_send)
    wait_for(zsum.at[pl.ds(0, planes - 1)], zsum_send)


def store_kernel(loglik, share, lengths, loglik_out, share_out, lengths_out, sem):
    copies = [
        pltpu.make_async_copy(loglik, loglik_out, sem.at[0]),
        pltpu.make_async_copy(share, share_out, sem.at[1]),
        pltpu.make_async_copy(lengths, lengths_out, sem.at[2]),
    ]
    for copy in copies:
        copy.start()
    for copy in copies:
        copy.wait()


def on_device(
    sizes,
    top_partial,
    bottom_partial,
    left_vectors,
    right_vectors,
    decay_rates,
    state_weights,
    part_rates,
    branch_lengths,
    pattern_weights,
    block_partition,
    chosen_branches,
):
    planes, across, doms, nblk, owned = sizes
    flat = BR * STATES * nblk
    group = across * doms
    hbm = pl.BlockSpec(memory_space=pltpu.HBM)
    vmem = pl.BlockSpec(memory_space=pltpu.VMEM)
    tree = branch_lengths.shape[0]
    loglik, share, lengths = pl.pallas_call(
        functools.partial(step_kernel, sizes),
        out_shape=(
            pltpu.VMEM((BR * nblk, BLK), F32),
            pltpu.VMEM((2, BR, owned), F32),
            pltpu.VMEM((tree,), F32),
        ),
        in_specs=[hbm] * 11,
        out_specs=(vmem, vmem, vmem),
        scratch_shapes=[
            pltpu.VMEM((flat + (ROWS - STATES) * nblk, BLK), F32),
            pltpu.VMEM((flat + (ROWS - STATES) * nblk, BLK), F32),
            pltpu.VMEM((nblk, BR // 2, 2 * ROWS, 2 * BLK), BF16),
            pltpu.VMEM((nblk, BR // 2, 2 * ROWS, 2 * BLK), BF16),
            pltpu.VMEM((nblk, ROWS, BLK), F32),
            pltpu.VMEM((ROWS, owned + 8, STATES), F32),
            pltpu.VMEM((ROWS, owned + 8, STATES), F32),
            pltpu.VMEM((owned, STATES), F32),
            pltpu.VMEM((owned, STATES), F32),
            pltpu.VMEM((nblk, BLK), jnp.int32),
            pltpu.SMEM((owned,), F32),
            pltpu.SMEM((tree,), F32),
            pltpu.SMEM((BR,), jnp.int32),
            pltpu.SMEM((1, nblk), jnp.int32),
            pltpu.VMEM((tree,), F32),
            pltpu.SMEM((doms - 1, 1, nblk), jnp.int32),
            pltpu.VMEM((2, nblk, ROWS, BLK), F32),
            pltpu.VMEM((2, nblk // 2, ROWS, BLK), F32),
            pltpu.VMEM((2, nblk, ROWS, BLK), F32),
            pltpu.VMEM((2, nblk // 2, ROWS, BLK), F32),
            pltpu.VMEM((2, 3, BR, BLK), F32),
            pltpu.VMEM((32 * nblk, BLK), F32),
            pltpu.VMEM((group, 4, BLK), F32),
            pltpu.VMEM((planes, BR + 1, BLK), F32),
            pltpu.SemaphoreType.DMA((12,)),
            pltpu.SemaphoreType.DMA,
            pltpu.SemaphoreType.DMA((doms - 1,)),
            pltpu.SemaphoreType.DMA,
            pltpu.SemaphoreType.DMA((nblk,)),
            pltpu.SemaphoreType.DMA,
            pltpu.SemaphoreType.DMA((nblk // 2,)),
            pltpu.SemaphoreType.DMA,
            pltpu.SemaphoreType.DMA,
            pltpu.SemaphoreType.DMA,
            pltpu.SemaphoreType.DMA,
            pltpu.SemaphoreType.REGULAR,
            pltpu.SemaphoreType.REGULAR,
            pltpu.SemaphoreType.REGULAR,
        ],
        compiler_params=pltpu.CompilerParams(
            collective_id=0, has_side_effects=True
        ),
    )(
        top_partial.reshape(BR, STATES, nblk, BLK).reshape(flat, BLK),
        bottom_partial.reshape(BR, STATES, nblk, BLK).reshape(flat, BLK),
        jnp.transpose(left_vectors, (1, 0, 2)),
        jnp.transpose(right_vectors, (1, 0, 2)),
        decay_rates,
        state_weights,
        part_rates,
        branch_lengths,
        chosen_branches,
        block_partition,
        pattern_weights.reshape(nblk, BLK),
    )
    loglik, share, new_lengths = pl.pallas_call(
        store_kernel,
        out_shape=(
            jax.ShapeDtypeStruct((BR * nblk, BLK), F32),
            jax.ShapeDtypeStruct((2, BR, owned), F32),
            jax.ShapeDtypeStruct((tree,), F32),
        ),
        in_specs=[vmem] * 3,
        out_specs=(hbm, hbm, hbm),
        scratch_shapes=[pltpu.SemaphoreType.DMA((3,))],
        compiler_params=pltpu.CompilerParams(vmem_limit_bytes=1024 * 1024),
    )(loglik, share, lengths)
    return (loglik.reshape(BR, 1, nblk * BLK), share, new_lengths)


def solution(mesh):
    sites, doms = mesh.shape["site"], mesh.shape["dom"]
    across = 8 if sites % 8 == 0 and sites > 8 else 2
    sizes = (sites // across, across, doms, 8, 256 // doms)
    return jax.shard_map(
        functools.partial(on_device, sizes),
        mesh=mesh,
        in_specs=(
            P(None, None, "dom", "site"),
            P(None, None, "dom", "site"),
            P("dom", None, None),
            P("dom", None, None),
            P("dom", None),
            P("dom", None),
            P("dom"),
            P(),
            P("dom", "site"),
            P("dom", "site"),
            P(),
        ),
        out_specs=(P(None, "dom", "site"), P(None, None, "dom"), P()),
        check_vma=False,
    )
```

```python
import functools

import jax
import jax.numpy as jnp
from jax import lax
from jax.experimental import pallas as pl
from jax.experimental.pallas import tpu as pltpu
from jax.sharding import PartitionSpec as P

BLK = 128
STATES = 61
ROWS = 64
BR = 16
F32 = jnp.float32
BF16 = jnp.bfloat16
MESH = pl.DeviceIdType.MESH


def hi_lo(x):
    hi = x.astype(BF16)
    return hi, (x - hi.astype(F32)).astype(BF16)


def three(x):
    hi = x.astype(BF16)
    rest = x - hi.astype(F32)
    mid = rest.astype(BF16)
    return hi, mid, (rest - mid.astype(F32)).astype(BF16)


def dot(a, b, contract):
    return lax.dot_general(a, b, ((contract[0], contract[1]), ((), ())), preferred_element_type=F32)


def step_kernel(
    sizes,
    top_hbm,
    bottom_hbm,
    left_hbm,
    right_hbm,
    decay_hbm,
    weight_hbm,
    rates_hbm,
    lengths_hbm,
    chosen_hbm,
    blocks_hbm,
    pattern_hbm,
    loglik_out,
    part_out,
    lengths_out,
    top,
    bottom,
    top_s,
    bottom_s,
    own_tab,
    left,
    right,
    decay,
    weight,
    pattern,
    rates,
    lengths,
    chosen,
    blocks,
    lengths_v,
    asked,
    near_tab,
    far_tab,
    recv_tab,
    relay,
    likes,
    sums,
    gath,
    numbers,
    hot,
    zsum,
    local_sem,
    ask_send,
    ask_recv,
    near_send,
    near_recv,
    far_send,
    far_recv,
    gath_send,
    gath_recv,
    num_send,
    num_recv,
    zsum_send,
    zsum_recv,
    line_sem,
    next_sem,
    after_sem,
):
    planes, across, doms, nblk, owned = sizes
    site = lax.axis_index("site")
    me = lax.axis_index("dom")
    plane = site // across
    column = site % across
    group = across * doms
    rank = column * doms + me
    def wait_for(ref, sem):
        pltpu.make_async_copy(ref, ref, sem).wait()

    dom_at = [me] + [lax.rem(me + off, doms) for off in range(1, doms)]
    dom_peer = lambda off: dom_at[off]
    site_at = [site] + [plane * across + lax.rem(column + off, across) for off in range(1, across)]
    plane_at = [site] + [lax.rem(plane + off, planes) * across + column for off in range(1, planes)]

    def group_peer(off):
        return {"site": site_at[off // doms], "dom": dom_at[off % doms]}

    def plane_peer(off):
        return {"site": plane_at[off], "dom": me}

    small = [
        pltpu.make_async_copy(blocks_hbm, blocks, local_sem.at[7]),
        pltpu.make_async_copy(rates_hbm, rates, local_sem.at[8]),
        pltpu.make_async_copy(chosen_hbm, chosen, local_sem.at[9]),
        pltpu.make_async_copy(lengths_hbm, lengths, local_sem.at[10]),
    ]
    small.append(pltpu.make_async_copy(lengths_hbm, lengths_v, local_sem.at[11]))
    small[0].start()
    loads = [
        pltpu.make_async_copy(left_hbm, left.at[pl.ds(0, STATES), pl.ds(0, owned)], local_sem.at[0]),
        pltpu.make_async_copy(right_hbm, right.at[pl.ds(0, STATES), pl.ds(0, owned)], local_sem.at[1]),
        pltpu.make_async_copy(decay_hbm, decay, local_sem.at[2]),
        pltpu.make_async_copy(weight_hbm, weight, local_sem.at[3]),
        pltpu.make_async_copy(pattern_hbm, pattern, local_sem.at[4]),
        pltpu.make_async_copy(top_hbm, top.at[pl.ds(0, BR * STATES * nblk)], local_sem.at[5]),
        pltpu.make_async_copy(bottom_hbm, bottom.at[pl.ds(0, BR * STATES * nblk)], local_sem.at[6]),
    ]
    for load in loads[:4] + small[1:] + loads[4:]:
        load.start()

    barrier = pltpu.get_barrier_semaphore()
    here = lambda s: {"site": s, "dom": me}
    near = [{"site": site, "dom": d} for d in dom_at[1:]]
    near += [here(s) for s in site_at[1:]] + [here(plane_at[1]), here(plane_at[planes - 1])]
    for device in near:
        pl.semaphore_signal(barrier, inc=1, device_id=device, device_id_type=MESH)

    small[0].wait()
    pl.semaphore_wait(barrier, len(near))

    def ask(off):
        return pltpu.make_async_remote_copy(
            src_ref=blocks,
            dst_ref=asked.at[off - 1],
            send_sem=ask_send,
            recv_sem=ask_recv.at[off - 1],
            device_id={"site": site, "dom": dom_peer(off)},
            device_id_type=MESH,
        )

    for off in range(1, doms):
        ask(off).start()

    pitch = left.shape[1]
    tail = (ROWS - STATES, pitch, STATES)
    left[pl.ds(STATES, ROWS - STATES)] = jnp.zeros(tail, F32)
    right[pl.ds(STATES, ROWS - STATES)] = jnp.zeros(tail, F32)
    left_rows = left.reshape((ROWS + 1) * pitch, STATES)
    right_rows = right.reshape((ROWS + 1) * pitch, STATES)
    tail = (ROWS - STATES) * nblk
    top[pl.ds(BR * STATES * nblk, tail), :] = jnp.zeros((tail, BLK), F32)
    bottom[pl.ds(BR * STATES * nblk, tail), :] = jnp.zeros((tail, BLK), F32)

    for s in site_at[1:]:
        pl.semaphore_signal(line_sem, inc=1, device_id=here(s), device_id_type=MESH)
    for off in (1, planes - 1):
        pl.semaphore_signal(next_sem, inc=1, device_id=here(plane_at[off]), device_id_type=MESH)

    row_id = lax.broadcasted_iota(jnp.int32, (ROWS, ROWS), 0)

    def entry(part):
        relative = part - me * owned
        inside = jnp.logical_and(relative >= 0, relative < owned).astype(F32)
        at = jnp.clip(relative, 0, owned - 1)
        lv = jnp.pad(left_rows[pl.ds(at, ROWS, stride=pitch), :], ((0, 0), (0, ROWS - STATES)))
        rv = jnp.pad(right_rows[pl.ds(at, ROWS, stride=pitch), :], ((0, 0), (0, ROWS - STATES)))
        pad = lambda x: jnp.pad(x, ((0, 0), (0, ROWS - STATES)))
        exponent = pad(-decay[pl.ds(at, 1), :] * rates[at])
        state_w = pad(weight[pl.ds(at, 1), :])
        lv = jnp.where(row_id == STATES, exponent, jnp.where(row_id == STATES + 1, state_w, lv))
        return jnp.concatenate([lv, rv], axis=1) * inside

    half = nblk // 2
    to_side = [dom_at[doms - 1], dom_at[1]]
    near_ids, far_ids = [0, doms - 2], 1

    def near(side, n):
        return pltpu.make_async_remote_copy(
            src_ref=near_tab.at[side, n],
            dst_ref=recv_tab.at[side, n],
            send_sem=near_send,
            recv_sem=near_recv.at[n],
            device_id={"site": site, "dom": to_side[side]},
            device_id_type=MESH,
        )

    def far(side, i):
        return pltpu.make_async_remote_copy(
            src_ref=far_tab.at[side, i],
            dst_ref=relay.at[side, i],
            send_sem=far_send,
            recv_sem=far_recv.at[i],
            device_id={"site": site, "dom": to_side[side]},
            device_id_type=MESH,
        )

    def direct(start, stop):
        @pl.loop(start, stop)
        def _(i):
            for side in range(2):
                n = (1 - side) * half + i
                near_tab[side, n] = entry(asked[near_ids[side], 0, n])
            for side in range(2):
                near(side, (1 - side) * half + i).start()

    def split(ref, out):
        @pl.loop(0, nblk)
        def _(n):
            for b in range(BR):
                hi, lo = hi_lo(ref[pl.ds(b * (STATES * nblk) + n, ROWS, stride=nblk), :])
                lanes = pl.ds((b % 2) * BLK, BLK)
                out[n, b // 2, pl.ds(0, ROWS), lanes] = hi
                out[n, b // 2, pl.ds(ROWS, ROWS), lanes] = lo

    def passed_on(start, stop):
        @pl.loop(start, stop)
        def _(i):
            mine = [entry(asked[near_ids[side], 0, side * half + i]) for side in range(2)]
            wait_for(relay.at[:, i], far_recv.at[i])
            for side in range(2):
                near_tab[side, side * half + i] = mine[side] + relay[side, i]
            for side in range(2):
                near(side, side * half + i).start()

    for load in loads[:4] + small[1:]:
        load.wait()
    ask(1).wait_recv()
    ask(doms - 1).wait_recv()
    direct(0, 1)
    ask(2).wait_recv()

    @pl.loop(0, half)
    def _(i):
        for side in range(2):
            far_tab[side, i] = entry(asked[far_ids, 0, side * half + i])
        for side in range(2):
            far(side, i).start()

    direct(1, half - 2)

    @pl.loop(0, nblk)
    def _(n):
        own_tab[n] = entry(blocks[0, n])

    for load in loads[4:]:
        load.wait()
    split(top, top_s)
    split(bottom, bottom_s)
    passed_on(0, 1)
    direct(half - 2, half - 1)
    passed_on(1, half - 1)
    direct(half - 1, half)
    passed_on(half - 1, half)

    pl.semaphore_wait(next_sem, 2)
    for off in (2, planes - 2):
        pl.semaphore_signal(after_sem, inc=1, device_id=here(plane_at[off]), device_id_type=MESH)

    def give(src, dst, sems, off):
        return pltpu.make_async_remote_copy(
            src_ref=src.at[rank],
            dst_ref=dst.at[rank],
            send_sem=sems[0],
            recv_sem=sems[1],
            device_id=group_peer(off),
            device_id_type=MESH,
        )

    hops = lambda off, count: min(off, count - off)
    spread_out = sorted(
        range(1, group),
        key=lambda off: -hops(off // doms // 2, across // 2) - hops(off % doms, doms),
    )

    pl.semaphore_wait(line_sem, across - 1)
    lane_blk = lax.broadcasted_iota(jnp.int32, (1, BLK), 1) // 32
    for g in range(2):
        ids = jnp.zeros((1, BLK), F32)
        for k in range(4):
            ids = jnp.where(lane_blk == k, blocks[0, g * 4 + k].astype(F32), ids)
        numbers[rank, pl.ds(g, 1), :] = ids
    for off in spread_out:
        give(numbers, numbers, (num_send, num_recv), off).start()

    lane1 = lax.broadcasted_iota(jnp.int32, (1, BLK), 1)
    times = jnp.zeros((1, BLK), F32)
    for b in range(BR):
        times = jnp.where(lane1 == b, lengths[chosen[b]], times)
    lane64 = lax.broadcasted_iota(jnp.int32, (ROWS, ROWS), 1)

    def prepared(n):
        got = own_tab[n]
        for side in range(2):
            got = got + recv_tab[side, n]
        lv_t = jnp.transpose(got[:, :ROWS])
        state_w = got[STATES + 1 : STATES + 2, :ROWS]
        exponent = lv_t[:, STATES : STATES + 1]
        lv_t = jnp.where(lane64 < STATES, lv_t * state_w, 0.0)
        lv_hi, lv_lo = hi_lo(lv_t)
        rv_hi, rv_lo = hi_lo(got[:, ROWS:])
        lhs_l = jnp.concatenate([lv_hi, lv_hi, lv_lo], axis=1)
        lhs_r = jnp.concatenate([rv_hi, rv_hi, rv_lo], axis=1)
        expo_b = jnp.broadcast_to(exponent, (ROWS, BLK))
        decays = jnp.exp(exponent * times)
        return lhs_l, lhs_r, expo_b, decays

    def two_branches(n, slot, b, lhs_l, lhs_r, expo_b, decays):
        x, y = top_s[n, b // 2], bottom_s[n, b // 2]
        x = jnp.concatenate([x, x[:ROWS]], axis=0)
        y = jnp.concatenate([y, y[:ROWS]], axis=0)
        joint = dot(lhs_l, x, ((1,), (0,))) * dot(lhs_r, y, ((1,), (0,)))
        for c in range(2):
            decayed = joint[:, c * BLK : (c + 1) * BLK] * decays[:, b + c : b + c + 1]
            for power in range(3):
                likes[slot, power, pl.ds(b + c, 1), :] = jnp.sum(decayed, axis=0, keepdims=True)
                if power < 2:
                    decayed = decayed * expo_b

    def finished(n, slot):
        like0, like1, like2 = (likes[slot, power] for power in range(3))
        first = like1 / like0
        second = like2 / like0 - first * first
        sites_w = pattern[pl.ds(n, 1), :].astype(F32)
        loglik_out[pl.ds(n, BR, stride=nblk), :] = sites_w * jnp.log(like0)
        sums[pl.ds(n * 32, BR), :] = sites_w * first
        sums[pl.ds(n * 32 + BR, BR), :] = sites_w * second

    @pl.loop(0, half)
    def _(i):
        for side in range(2):
            wait_for(recv_tab.at[:, side * half + i], near_recv.at[side * half + i])
        tables = [prepared(side * half + i) for side in range(2)]
        for b in range(0, BR, 2):
            for side in range(2):
                two_branches(side * half + i, side, b, *tables[side])
        for side in range(2):
            finished(side * half + i, side)

    pl.semaphore_wait(after_sem, 2)

    ones = jnp.ones((8, BLK), BF16)
    total = sum(dot(ones, piece, ((1,), (1,))) for piece in three(sums[...]))
    for g in range(2):
        gath[rank, pl.ds(g, 1), :] = total[0:1, g * BLK : (g + 1) * BLK]
    for off in spread_out:
        give(gath, gath, (gath_send, gath_recv), off).start()

    wait_for(numbers.at[pl.ds(0, group - 1)], num_recv)
    ids = jnp.concatenate([numbers[:, 0, :], numbers[:, 1, :]], axis=0)
    local = lax.broadcasted_iota(jnp.int32, (2 * group, BLK), 1)
    mine = jnp.where(local < owned, local + me * owned, -1).astype(F32)
    for k in range(4):
        one = (ids[:, k * 32 : k * 32 + 1] == mine).astype(F32).astype(BF16)
        for copy in range(3):
            hot[pl.ds(copy * 2 * group, 2 * group), pl.ds(k * BLK, BLK)] = one

    wait_for(gath.at[pl.ds(0, group - 1)], gath_recv)
    vals = jnp.concatenate([gath[:, 0, :], gath[:, 1, :]], axis=0)
    vals_t = jnp.transpose(vals)
    spread = dot(
        jnp.concatenate(three(vals_t), axis=1),
        hot[...],
        ((1,), (0,)),
    )
    by_part = sum(spread[k * 32 : (k + 1) * 32, k * BLK : (k + 1) * BLK] for k in range(4))
    lane = lax.broadcasted_iota(jnp.int32, (BR, BLK), 1)
    zsum[plane, 0:BR, :] = jnp.where(
        lane < owned, by_part[:BR], pltpu.roll(by_part[BR:], owned, 1)
    )
    column_sum = jnp.sum(vals, axis=0, keepdims=True)
    all_sum = column_sum
    for k in range(1, 4):
        all_sum = all_sum + pltpu.roll(column_sum, 32 * k, 1)
    zsum[plane, BR : BR + 1, :] = all_sum

    def pass_on(off):
        return pltpu.make_async_remote_copy(
            src_ref=zsum.at[plane],
            dst_ref=zsum.at[plane],
            send_sem=zsum_send,
            recv_sem=zsum_recv,
            device_id=plane_peer(off),
            device_id_type=MESH,
        )

    for off in sorted(range(1, planes), key=lambda off: -hops(off, planes)):
        pass_on(off).start()

    wait_for(zsum.at[pl.ds(0, planes - 1)], zsum_recv)

    done = jnp.sum(zsum[...], axis=0)
    both = done[:BR]
    part_out[0] = both[:, :owned]
    part_out[1] = pltpu.roll(both, owned, 1)[:, :owned]
    totals = jnp.broadcast_to(done[BR : BR + 1], (8, BLK))
    updated = times - totals / pltpu.roll(totals, BLK - BR, 1)
    tree = lengths_v.shape[0]
    index = lax.broadcasted_iota(jnp.int32, (1, BLK), 1)
    spots = [jnp.broadcast_to(updated[0:1, b : b + 1], (1, BLK)) for b in range(BR)]
    for start in range(0, tree, BLK):
        width = min(BLK, tree - start)
        new = lengths_v[pl.ds(start, width)].reshape(1, width)
        for b in range(BR):
            new = jnp.where(index[:, :width] + start == chosen[b], spots[b][:, :width], new)
        lengths_out[pl.ds(start, width)] = new.reshape(width)

    wait_for(asked, ask_send)
    wait_for(near_tab, near_send)
    wait_for(far_tab, far_send)
    wait_for(gath.at[pl.ds(0, group - 1)], gath_send)
    wait_for(numbers.at[pl.ds(0, group - 1)], num_send)
    wait_for(zsum.at[pl.ds(0, planes - 1)], zsum_send)


def store_kernel(loglik, share, lengths, loglik_out, share_out, lengths_out, sem):
    copies = [
        pltpu.make_async_copy(loglik, loglik_out, sem.at[0]),
        pltpu.make_async_copy(share, share_out, sem.at[1]),
        pltpu.make_async_copy(lengths, lengths_out, sem.at[2]),
    ]
    for copy in copies:
        copy.start()
    for copy in copies:
        copy.wait()


def on_device(
    sizes,
    top_partial,
    bottom_partial,
    left_vectors,
    right_vectors,
    decay_rates,
    state_weights,
    part_rates,
    branch_lengths,
    pattern_weights,
    block_partition,
    chosen_branches,
):
    planes, across, doms, nblk, owned = sizes
    flat = BR * STATES * nblk
    group = across * doms
    hbm = pl.BlockSpec(memory_space=pltpu.HBM)
    vmem = pl.BlockSpec(memory_space=pltpu.VMEM)
    tree = branch_lengths.shape[0]
    loglik, share, lengths = pl.pallas_call(
        functools.partial(step_kernel, sizes),
        out_shape=(
            pltpu.VMEM((BR * nblk, BLK), F32),
            pltpu.VMEM((2, BR, owned), F32),
            pltpu.VMEM((tree,), F32),
        ),
        in_specs=[hbm] * 11,
        out_specs=(vmem, vmem, vmem),
        scratch_shapes=[
            pltpu.VMEM((flat + (ROWS - STATES + 1) * nblk, BLK), F32),
            pltpu.VMEM((flat + (ROWS - STATES + 1) * nblk, BLK), F32),
            pltpu.VMEM((nblk, BR // 2, 2 * ROWS, 2 * BLK), BF16),
            pltpu.VMEM((nblk, BR // 2, 2 * ROWS, 2 * BLK), BF16),
            pltpu.VMEM((nblk, ROWS, BLK), F32),
            pltpu.VMEM((ROWS + 1, owned + 8, STATES), F32),
            pltpu.VMEM((ROWS + 1, owned + 8, STATES), F32),
            pltpu.VMEM((owned, STATES), F32),
            pltpu.VMEM((owned, STATES), F32),
            pltpu.VMEM((nblk, BLK), jnp.int32),
            pltpu.SMEM((owned,), F32),
            pltpu.SMEM((tree,), F32),
            pltpu.SMEM((BR,), jnp.int32),
            pltpu.SMEM((1, nblk), jnp.int32),
            pltpu.VMEM((tree,), F32),
            pltpu.SMEM((doms - 1, 1, nblk), jnp.int32),
            pltpu.VMEM((2, nblk, ROWS, BLK), F32),
            pltpu.VMEM((2, nblk // 2, ROWS, BLK), F32),
            pltpu.VMEM((2, nblk, ROWS, BLK), F32),
            pltpu.VMEM((2, nblk // 2, ROWS, BLK), F32),
            pltpu.VMEM((2, 3, BR, BLK), F32),
            pltpu.VMEM((32 * nblk, BLK), F32),
            pltpu.VMEM((group, 2, BLK), F32),
            pltpu.VMEM((group, 2, BLK), F32),
            pltpu.VMEM((6 * group, 4 * BLK), BF16),
            pltpu.VMEM((planes, BR + 1, BLK), F32),
            pltpu.SemaphoreType.DMA((12,)),
            pltpu.SemaphoreType.DMA,
            pltpu.SemaphoreType.DMA((doms - 1,)),
            pltpu.SemaphoreType.DMA,
            pltpu.SemaphoreType.DMA((nblk,)),
            pltpu.SemaphoreType.DMA,
            pltpu.SemaphoreType.DMA((nblk // 2,)),
            pltpu.SemaphoreType.DMA,
            pltpu.SemaphoreType.DMA,
            pltpu.SemaphoreType.DMA,
            pltpu.SemaphoreType.DMA,
            pltpu.SemaphoreType.DMA,
            pltpu.SemaphoreType.DMA,
            pltpu.SemaphoreType.REGULAR,
            pltpu.SemaphoreType.REGULAR,
            pltpu.SemaphoreType.REGULAR,
        ],
        compiler_params=pltpu.CompilerParams(
            collective_id=0, has_side_effects=True
        ),
    )(
        top_partial.reshape(BR, STATES, nblk, BLK).reshape(flat, BLK),
        bottom_partial.reshape(BR, STATES, nblk, BLK).reshape(flat, BLK),
        jnp.transpose(left_vectors, (1, 0, 2)),
        jnp.transpose(right_vectors, (1, 0, 2)),
        decay_rates,
        state_weights,
        part_rates,
        branch_lengths,
        chosen_branches,
        block_partition,
        pattern_weights.reshape(nblk, BLK),
    )
    loglik, share, new_lengths = pl.pallas_call(
        store_kernel,
        out_shape=(
            jax.ShapeDtypeStruct((BR * nblk, BLK), F32),
            jax.ShapeDtypeStruct((2, BR, owned), F32),
            jax.ShapeDtypeStruct((tree,), F32),
        ),
        in_specs=[vmem] * 3,
        out_specs=(hbm, hbm, hbm),
        scratch_shapes=[pltpu.SemaphoreType.DMA((3,))],
        compiler_params=pltpu.CompilerParams(vmem_limit_bytes=1024 * 1024),
    )(loglik, share, lengths)
    return (loglik.reshape(BR, 1, nblk * BLK), share, new_lengths)


def solution(mesh):
    sites, doms = mesh.shape["site"], mesh.shape["dom"]
    across = 8 if sites % 8 == 0 and sites > 8 else 2
    sizes = (sites // across, across, doms, 8, 256 // doms)
    return jax.shard_map(
        functools.partial(on_device, sizes),
        mesh=mesh,
        in_specs=(
            P(None, None, "dom", "site"),
            P(None, None, "dom", "site"),
            P("dom", None, None),
            P("dom", None, None),
            P("dom", None),
            P("dom", None),
            P("dom"),
            P(),
            P("dom", "site"),
            P("dom", "site"),
            P(),
        ),
        out_specs=(P(None, "dom", "site"), P(None, None, "dom"), P()),
        check_vma=False,
    )
```

```python
import functools

import jax
import jax.numpy as jnp
from jax import lax
from jax.experimental import pallas as pl
from jax.experimental.pallas import tpu as pltpu
from jax.sharding import PartitionSpec as P

BLK = 128
STATES = 61
ROWS = 64
BR = 16
F32 = jnp.float32
BF16 = jnp.bfloat16
MESH = pl.DeviceIdType.MESH


def hi_lo(x):
    hi = x.astype(BF16)
    return hi, (x - hi.astype(F32)).astype(BF16)


def three(x):
    hi = x.astype(BF16)
    rest = x - hi.astype(F32)
    mid = rest.astype(BF16)
    return hi, mid, (rest - mid.astype(F32)).astype(BF16)


def dot(a, b, contract):
    return lax.dot_general(a, b, ((contract[0], contract[1]), ((), ())), preferred_element_type=F32)


def step_kernel(
    sizes,
    top_hbm,
    bottom_hbm,
    left_hbm,
    right_hbm,
    decay_hbm,
    weight_hbm,
    rates_hbm,
    lengths_hbm,
    chosen_hbm,
    blocks_hbm,
    pattern_hbm,
    loglik_out,
    part_out,
    lengths_out,
    top,
    bottom,
    top_s,
    bottom_s,
    own_tab,
    left,
    right,
    decay,
    weight,
    pattern,
    rates,
    lengths,
    chosen,
    blocks,
    lengths_v,
    asked,
    near_tab,
    far_tab,
    recv_tab,
    relay,
    likes,
    sums,
    gath,
    numbers,
    hot,
    zsum,
    local_sem,
    ask_send,
    ask_recv,
    near_send,
    near_recv,
    far_send,
    far_recv,
    gath_send,
    gath_recv,
    num_send,
    num_recv,
    zsum_send,
    zsum_recv,
    line_sem,
    next_sem,
    after_sem,
):
    planes, across, doms, nblk, owned = sizes
    site = lax.axis_index("site")
    me = lax.axis_index("dom")
    plane = site // across
    column = site % across
    group = across * doms
    rank = column * doms + me
    def wait_for(ref, sem):
        pltpu.make_async_copy(ref, ref, sem).wait()

    dom_at = [me] + [lax.rem(me + off, doms) for off in range(1, doms)]
    dom_peer = lambda off: dom_at[off]
    site_at = [site] + [plane * across + lax.rem(column + off, across) for off in range(1, across)]
    plane_at = [site] + [lax.rem(plane + off, planes) * across + column for off in range(1, planes)]

    def group_peer(off):
        return {"site": site_at[off // doms], "dom": dom_at[off % doms]}

    def plane_peer(off):
        return {"site": plane_at[off], "dom": me}

    small = [
        pltpu.make_async_copy(blocks_hbm, blocks, local_sem.at[7]),
        pltpu.make_async_copy(rates_hbm, rates, local_sem.at[8]),
        pltpu.make_async_copy(chosen_hbm, chosen, local_sem.at[9]),
        pltpu.make_async_copy(lengths_hbm, lengths, local_sem.at[10]),
    ]
    small.append(pltpu.make_async_copy(lengths_hbm, lengths_v, local_sem.at[11]))
    small[0].start()
    loads = [
        pltpu.make_async_copy(left_hbm, left.at[pl.ds(0, STATES), pl.ds(0, owned)], local_sem.at[0]),
        pltpu.make_async_copy(right_hbm, right.at[pl.ds(0, STATES), pl.ds(0, owned)], local_sem.at[1]),
        pltpu.make_async_copy(decay_hbm, decay, local_sem.at[2]),
        pltpu.make_async_copy(weight_hbm, weight, local_sem.at[3]),
        pltpu.make_async_copy(pattern_hbm, pattern, local_sem.at[4]),
        pltpu.make_async_copy(top_hbm, top.at[pl.ds(0, BR * STATES * nblk)], local_sem.at[5]),
        pltpu.make_async_copy(bottom_hbm, bottom.at[pl.ds(0, BR * STATES * nblk)], local_sem.at[6]),
    ]
    for load in loads[:4] + small[1:] + loads[4:]:
        load.start()

    barrier = pltpu.get_barrier_semaphore()
    here = lambda s: {"site": s, "dom": me}
    near = [{"site": site, "dom": d} for d in dom_at[1:]]
    near += [here(s) for s in site_at[1:]] + [here(plane_at[1]), here(plane_at[planes - 1])]
    for device in near:
        pl.semaphore_signal(barrier, inc=1, device_id=device, device_id_type=MESH)

    small[0].wait()
    pl.semaphore_wait(barrier, len(near))

    def ask(off):
        return pltpu.make_async_remote_copy(
            src_ref=blocks,
            dst_ref=asked.at[off - 1],
            send_sem=ask_send,
            recv_sem=ask_recv.at[off - 1],
            device_id={"site": site, "dom": dom_peer(off)},
            device_id_type=MESH,
        )

    for off in range(1, doms):
        ask(off).start()

    pitch = left.shape[1]
    tail = (ROWS - STATES, pitch, STATES)
    left[pl.ds(STATES, ROWS - STATES)] = jnp.zeros(tail, F32)
    right[pl.ds(STATES, ROWS - STATES)] = jnp.zeros(tail, F32)
    left_rows = left.reshape((ROWS + 1) * pitch, STATES)
    right_rows = right.reshape((ROWS + 1) * pitch, STATES)
    tail = (ROWS - STATES) * nblk
    top[pl.ds(BR * STATES * nblk, tail), :] = jnp.zeros((tail, BLK), F32)
    bottom[pl.ds(BR * STATES * nblk, tail), :] = jnp.zeros((tail, BLK), F32)

    for s in site_at[1:]:
        pl.semaphore_signal(line_sem, inc=1, device_id=here(s), device_id_type=MESH)
    for off in (1, planes - 1):
        pl.semaphore_signal(next_sem, inc=1, device_id=here(plane_at[off]), device_id_type=MESH)

    row_id = lax.broadcasted_iota(jnp.int32, (ROWS, ROWS), 0)

    def entry(part):
        relative = part - me * owned
        inside = jnp.logical_and(relative >= 0, relative < owned).astype(F32)
        at = jnp.clip(relative, 0, owned - 1)
        lv = jnp.pad(left_rows[pl.ds(at, ROWS, stride=pitch), :], ((0, 0), (0, ROWS - STATES)))
        rv = jnp.pad(right_rows[pl.ds(at, ROWS, stride=pitch), :], ((0, 0), (0, ROWS - STATES)))
        pad = lambda x: jnp.pad(x, ((0, 0), (0, ROWS - STATES)))
        exponent = pad(-decay[pl.ds(at, 1), :] * rates[at])
        state_w = pad(weight[pl.ds(at, 1), :])
        lv = jnp.where(row_id == STATES, exponent, jnp.where(row_id == STATES + 1, state_w, lv))
        return jnp.concatenate([lv, rv], axis=1) * inside

    half = nblk // 2
    to_side = [dom_at[doms - 1], dom_at[1]]
    near_ids, far_ids = [0, doms - 2], 1

    def near(side, n):
        return pltpu.make_async_remote_copy(
            src_ref=near_tab.at[side, n],
            dst_ref=recv_tab.at[side, n],
            send_sem=near_send,
            recv_sem=near_recv.at[n],
            device_id={"site": site, "dom": to_side[side]},
            device_id_type=MESH,
        )

    def far(side, i):
        return pltpu.make_async_remote_copy(
            src_ref=far_tab.at[side, i],
            dst_ref=relay.at[side, i],
            send_sem=far_send,
            recv_sem=far_recv.at[i],
            device_id={"site": site, "dom": to_side[side]},
            device_id_type=MESH,
        )

    def direct(start, stop):
        @pl.loop(start, stop)
        def _(i):
            for side in range(2):
                n = (1 - side) * half + i
                near_tab[side, n] = entry(asked[near_ids[side], 0, n])
            for side in range(2):
                near(side, (1 - side) * half + i).start()

    def split(ref, out):
        @pl.loop(0, nblk)
        def _(n):
            for b in range(BR):
                hi, lo = hi_lo(ref[pl.ds(b * (STATES * nblk) + n, ROWS, stride=nblk), :])
                lanes = pl.ds((b % 2) * BLK, BLK)
                out[n, b // 2, pl.ds(0, ROWS), lanes] = hi
                out[n, b // 2, pl.ds(ROWS, ROWS), lanes] = lo

    def passed_on(start, stop):
        @pl.loop(start, stop)
        def _(i):
            mine = [entry(asked[near_ids[side], 0, side * half + i]) for side in range(2)]
            wait_for(relay.at[:, i], far_recv.at[i])
            for side in range(2):
                near_tab[side, side * half + i] = mine[side] + relay[side, i]
            for side in range(2):
                near(side, side * half + i).start()

    for load in loads[:4] + small[1:]:
        load.wait()
    for side, off in ((0, 1), (1, doms - 1)):
        ask(off).wait_recv()
        n = (1 - side) * half
        near_tab[side, n] = entry(asked[near_ids[side], 0, n])
        near(side, n).start()
    ask(2).wait_recv()

    @pl.loop(0, half)
    def _(i):
        for side in range(2):
            far_tab[side, i] = entry(asked[far_ids, 0, side * half + i])
        for side in range(2):
            far(side, i).start()

    direct(1, half - 2)

    @pl.loop(0, nblk)
    def _(n):
        own_tab[n] = entry(blocks[0, n])

    for load in loads[4:]:
        load.wait()
    split(top, top_s)
    split(bottom, bottom_s)
    passed_on(0, 1)
    direct(half - 2, half - 1)
    passed_on(1, half - 1)
    direct(half - 1, half)
    passed_on(half - 1, half)

    pl.semaphore_wait(next_sem, 2)
    for off in (2, planes - 2):
        pl.semaphore_signal(after_sem, inc=1, device_id=here(plane_at[off]), device_id_type=MESH)

    def give(src, dst, sems, off):
        return pltpu.make_async_remote_copy(
            src_ref=src.at[rank],
            dst_ref=dst.at[rank],
            send_sem=sems[0],
            recv_sem=sems[1],
            device_id=group_peer(off),
            device_id_type=MESH,
        )

    hops = lambda off, count: min(off, count - off)
    spread_out = sorted(
        range(1, group),
        key=lambda off: -hops(off // doms // 2, across // 2) - hops(off % doms, doms),
    )

    pl.semaphore_wait(line_sem, across - 1)
    lane_blk = lax.broadcasted_iota(jnp.int32, (1, BLK), 1) // 32
    for g in range(2):
        ids = jnp.zeros((1, BLK), F32)
        for k in range(4):
            ids = jnp.where(lane_blk == k, blocks[0, g * 4 + k].astype(F32), ids)
        numbers[rank, pl.ds(g, 1), :] = ids
    for off in spread_out:
        give(numbers, numbers, (num_send, num_recv), off).start()

    lane1 = lax.broadcasted_iota(jnp.int32, (1, BLK), 1)
    times = jnp.zeros((1, BLK), F32)
    for b in range(BR):
        times = jnp.where(lane1 == b, lengths[chosen[b]], times)
    lane64 = lax.broadcasted_iota(jnp.int32, (ROWS, ROWS), 1)

    def prepared(n):
        got = own_tab[n]
        for side in range(2):
            got = got + recv_tab[side, n]
        lv_t = jnp.transpose(got[:, :ROWS])
        state_w = got[STATES + 1 : STATES + 2, :ROWS]
        exponent = lv_t[:, STATES : STATES + 1]
        lv_t = jnp.where(lane64 < STATES, lv_t * state_w, 0.0)
        lv_hi, lv_lo = hi_lo(lv_t)
        rv_hi, rv_lo = hi_lo(got[:, ROWS:])
        lhs_l = jnp.concatenate([lv_hi, lv_hi, lv_lo], axis=1)
        lhs_r = jnp.concatenate([rv_hi, rv_hi, rv_lo], axis=1)
        expo_b = jnp.broadcast_to(exponent, (ROWS, BLK))
        decays = jnp.exp(exponent * times)
        return lhs_l, lhs_r, expo_b, decays

    def two_branches(n, slot, b, lhs_l, lhs_r, expo_b, decays):
        x, y = top_s[n, b // 2], bottom_s[n, b // 2]
        x = jnp.concatenate([x, x[:ROWS]], axis=0)
        y = jnp.concatenate([y, y[:ROWS]], axis=0)
        joint = dot(lhs_l, x, ((1,), (0,))) * dot(lhs_r, y, ((1,), (0,)))
        for c in range(2):
            decayed = joint[:, c * BLK : (c + 1) * BLK] * decays[:, b + c : b + c + 1]
            for power in range(3):
                likes[slot, power, pl.ds(b + c, 1), :] = jnp.sum(decayed, axis=0, keepdims=True)
                if power < 2:
                    decayed = decayed * expo_b

    def finished(n, slot):
        like0, like1, like2 = (likes[slot, power] for power in range(3))
        first = like1 / like0
        second = like2 / like0 - first * first
        sites_w = pattern[pl.ds(n, 1), :].astype(F32)
        loglik_out[pl.ds(n, BR, stride=nblk), :] = sites_w * jnp.log(like0)
        sums[pl.ds(n * 32, BR), :] = sites_w * first
        sums[pl.ds(n * 32 + BR, BR), :] = sites_w * second

    @pl.loop(0, half)
    def _(i):
        for side in range(2):
            wait_for(recv_tab.at[:, side * half + i], near_recv.at[side * half + i])
        tables = [prepared(side * half + i) for side in range(2)]
        for b in range(0, BR, 2):
            for side in range(2):
                two_branches(side * half + i, side, b, *tables[side])
        for side in range(2):
            finished(side * half + i, side)

    pl.semaphore_wait(after_sem, 2)

    ones = jnp.ones((8, BLK), BF16)
    total = sum(dot(ones, piece, ((1,), (1,))) for piece in three(sums[...]))
    for g in range(2):
        gath[rank, pl.ds(g, 1), :] = total[0:1, g * BLK : (g + 1) * BLK]
    for off in spread_out:
        give(gath, gath, (gath_send, gath_recv), off).start()

    wait_for(numbers.at[pl.ds(0, group - 1)], num_recv)
    ids = jnp.concatenate([numbers[:, 0, :], numbers[:, 1, :]], axis=0)
    local = lax.broadcasted_iota(jnp.int32, (2 * group, BLK), 1)
    mine = jnp.where(local < owned, local + me * owned, -1).astype(F32)
    for k in range(4):
        one = (ids[:, k * 32 : k * 32 + 1] == mine).astype(F32).astype(BF16)
        for copy in range(3):
            hot[pl.ds(copy * 2 * group, 2 * group), pl.ds(k * BLK, BLK)] = one

    wait_for(gath.at[pl.ds(0, group - 1)], gath_recv)
    vals = jnp.concatenate([gath[:, 0, :], gath[:, 1, :]], axis=0)
    vals_t = jnp.transpose(vals)
    spread = dot(
        jnp.concatenate(three(vals_t), axis=1),
        hot[...],
        ((1,), (0,)),
    )
    by_part = sum(spread[k * 32 : (k + 1) * 32, k * BLK : (k + 1) * BLK] for k in range(4))
    lane = lax.broadcasted_iota(jnp.int32, (BR, BLK), 1)
    zsum[plane, 0:BR, :] = jnp.where(
        lane < owned, by_part[:BR], pltpu.roll(by_part[BR:], owned, 1)
    )
    column_sum = jnp.sum(vals, axis=0, keepdims=True)
    all_sum = column_sum
    for k in range(1, 4):
        all_sum = all_sum + pltpu.roll(column_sum, 32 * k, 1)
    zsum[plane, BR : BR + 1, :] = all_sum

    def pass_on(off):
        return pltpu.make_async_remote_copy(
            src_ref=zsum.at[plane],
            dst_ref=zsum.at[plane],
            send_sem=zsum_send,
            recv_sem=zsum_recv,
            device_id=plane_peer(off),
            device_id_type=MESH,
        )

    for off in sorted(range(1, planes), key=lambda off: -hops(off, planes)):
        pass_on(off).start()

    wait_for(zsum.at[pl.ds(0, planes - 1)], zsum_recv)

    done = jnp.sum(zsum[...], axis=0)
    both = done[:BR]
    part_out[0] = both[:, :owned]
    part_out[1] = pltpu.roll(both, owned, 1)[:, :owned]
    totals = jnp.broadcast_to(done[BR : BR + 1], (8, BLK))
    updated = times - totals / pltpu.roll(totals, BLK - BR, 1)
    tree = lengths_v.shape[0]
    index = lax.broadcasted_iota(jnp.int32, (1, BLK), 1)
    spots = [jnp.broadcast_to(updated[0:1, b : b + 1], (1, BLK)) for b in range(BR)]
    for start in range(0, tree, BLK):
        width = min(BLK, tree - start)
        new = lengths_v[pl.ds(start, width)].reshape(1, width)
        for b in range(BR):
            new = jnp.where(index[:, :width] + start == chosen[b], spots[b][:, :width], new)
        lengths_out[pl.ds(start, width)] = new.reshape(width)

    wait_for(asked, ask_send)
    wait_for(near_tab, near_send)
    wait_for(far_tab, far_send)
    wait_for(gath.at[pl.ds(0, group - 1)], gath_send)
    wait_for(numbers.at[pl.ds(0, group - 1)], num_send)
    wait_for(zsum.at[pl.ds(0, planes - 1)], zsum_send)


def store_kernel(loglik, share, lengths, loglik_out, share_out, lengths_out, sem):
    copies = [
        pltpu.make_async_copy(loglik, loglik_out, sem.at[0]),
        pltpu.make_async_copy(share, share_out, sem.at[1]),
        pltpu.make_async_copy(lengths, lengths_out, sem.at[2]),
    ]
    for copy in copies:
        copy.start()
    for copy in copies:
        copy.wait()


def on_device(
    sizes,
    top_partial,
    bottom_partial,
    left_vectors,
    right_vectors,
    decay_rates,
    state_weights,
    part_rates,
    branch_lengths,
    pattern_weights,
    block_partition,
    chosen_branches,
):
    planes, across, doms, nblk, owned = sizes
    flat = BR * STATES * nblk
    group = across * doms
    hbm = pl.BlockSpec(memory_space=pltpu.HBM)
    vmem = pl.BlockSpec(memory_space=pltpu.VMEM)
    tree = branch_lengths.shape[0]
    loglik, share, lengths = pl.pallas_call(
        functools.partial(step_kernel, sizes),
        out_shape=(
            pltpu.VMEM((BR * nblk, BLK), F32),
            pltpu.VMEM((2, BR, owned), F32),
            pltpu.VMEM((tree,), F32),
        ),
        in_specs=[hbm] * 11,
        out_specs=(vmem, vmem, vmem),
        scratch_shapes=[
            pltpu.VMEM((flat + (ROWS - STATES + 1) * nblk, BLK), F32),
            pltpu.VMEM((flat + (ROWS - STATES + 1) * nblk, BLK), F32),
            pltpu.VMEM((nblk, BR // 2, 2 * ROWS, 2 * BLK), BF16),
            pltpu.VMEM((nblk, BR // 2, 2 * ROWS, 2 * BLK), BF16),
            pltpu.VMEM((nblk, ROWS, BLK), F32),
            pltpu.VMEM((ROWS + 1, owned + 8, STATES), F32),
            pltpu.VMEM((ROWS + 1, owned + 8, STATES), F32),
            pltpu.VMEM((owned, STATES), F32),
            pltpu.VMEM((owned, STATES), F32),
            pltpu.VMEM((nblk, BLK), jnp.int32),
            pltpu.SMEM((owned,), F32),
            pltpu.SMEM((tree,), F32),
            pltpu.SMEM((BR,), jnp.int32),
            pltpu.SMEM((1, nblk), jnp.int32),
            pltpu.VMEM((tree,), F32),
            pltpu.SMEM((doms - 1, 1, nblk), jnp.int32),
            pltpu.VMEM((2, nblk, ROWS, BLK), F32),
            pltpu.VMEM((2, nblk // 2, ROWS, BLK), F32),
            pltpu.VMEM((2, nblk, ROWS, BLK), F32),
            pltpu.VMEM((2, nblk // 2, ROWS, BLK), F32),
            pltpu.VMEM((2, 3, BR, BLK), F32),
            pltpu.VMEM((32 * nblk, BLK), F32),
            pltpu.VMEM((group, 2, BLK), F32),
            pltpu.VMEM((group, 2, BLK), F32),
            pltpu.VMEM((6 * group, 4 * BLK), BF16),
            pltpu.VMEM((planes, BR + 1, BLK), F32),
            pltpu.SemaphoreType.DMA((12,)),
            pltpu.SemaphoreType.DMA,
            pltpu.SemaphoreType.DMA((doms - 1,)),
            pltpu.SemaphoreType.DMA,
            pltpu.SemaphoreType.DMA((nblk,)),
            pltpu.SemaphoreType.DMA,
            pltpu.SemaphoreType.DMA((nblk // 2,)),
            pltpu.SemaphoreType.DMA,
            pltpu.SemaphoreType.DMA,
            pltpu.SemaphoreType.DMA,
            pltpu.SemaphoreType.DMA,
            pltpu.SemaphoreType.DMA,
            pltpu.SemaphoreType.DMA,
            pltpu.SemaphoreType.REGULAR,
            pltpu.SemaphoreType.REGULAR,
            pltpu.SemaphoreType.REGULAR,
        ],
        compiler_params=pltpu.CompilerParams(
            collective_id=0, has_side_effects=True
        ),
    )(
        top_partial.reshape(BR, STATES, nblk, BLK).reshape(flat, BLK),
        bottom_partial.reshape(BR, STATES, nblk, BLK).reshape(flat, BLK),
        jnp.transpose(left_vectors, (1, 0, 2)),
        jnp.transpose(right_vectors, (1, 0, 2)),
        decay_rates,
        state_weights,
        part_rates,
        branch_lengths,
        chosen_branches,
        block_partition,
        pattern_weights.reshape(nblk, BLK),
    )
    loglik, share, new_lengths = pl.pallas_call(
        store_kernel,
        out_shape=(
            jax.ShapeDtypeStruct((BR * nblk, BLK), F32),
            jax.ShapeDtypeStruct((2, BR, owned), F32),
            jax.ShapeDtypeStruct((tree,), F32),
        ),
        in_specs=[vmem] * 3,
        out_specs=(hbm, hbm, hbm),
        scratch_shapes=[pltpu.SemaphoreType.DMA((3,))],
        compiler_params=pltpu.CompilerParams(vmem_limit_bytes=1024 * 1024),
    )(loglik, share, lengths)
    return (loglik.reshape(BR, 1, nblk * BLK), share, new_lengths)


def solution(mesh):
    sites, doms = mesh.shape["site"], mesh.shape["dom"]
    across = 8 if sites % 8 == 0 and sites > 8 else 2
    sizes = (sites // across, across, doms, 8, 256 // doms)
    return jax.shard_map(
        functools.partial(on_device, sizes),
        mesh=mesh,
        in_specs=(
            P(None, None, "dom", "site"),
            P(None, None, "dom", "site"),
            P("dom", None, None),
            P("dom", None, None),
            P("dom", None),
            P("dom", None),
            P("dom"),
            P(),
            P("dom", "site"),
            P("dom", "site"),
            P(),
        ),
        out_specs=(P(None, "dom", "site"), P(None, None, "dom"), P()),
        check_vma=False,
    )
```
